32 devices in a mesh: row: 4 (over z), col: 2 (over y), layer: 4 (over x, core).
Axes of the slice: x: 2, y: 2, z: 4, core: 2. Of those that a mesh axis runs over, the one named last changes fastest.
Arguments:
- amplitudes: float32 [2016, 73536], P('row', ('layer', 'col')), may hold values from -6 to 6
- integrals: float32 [73536, 768], P(('layer', 'col'), 'row'), may hold values from -0.03125 to 0.03125
- occ_energy: float32 [64], replicated, may hold values from -2 to -0.5
- vir_energy: float32 [384], replicated, may hold values from 0.2 to 3
Outputs:
- ladder: float32 [2016, 768], P('col', ('row', 'layer'))
- amplitude_step: float32 [2016, 768], P('col', ('row', 'layer'))
The draws below stay inside these ranges and needn't reach their ends.
All inputs are finite; a program needn't handle non-finite values.
Results may differ from the reference program's by a relative error of at most 0.00007.
Values sent between devices are 32-bit elements; how exact they have to be, the bound alone decides.
A program may use at most 128 MiB of HBM per device.

```python
import jax
import jax.numpy as jnp
import numpy as np
from jax import lax

NO = 64
NV = 384
IJ = 2016
K = 73536
AB = 768


def spiked(values, stream_key, source, target, parts, factor):
    def block_of(dim):
        return (jnp.arange(values.shape[dim]) // (values.shape[dim] // parts)).reshape((-1,) + (1,) * (values.ndim - 1 - dim))

    one_side = jax.random.permutation(stream_key, parts)[block_of(target)]
    far = (block_of(target) + parts // 2) % parts
    return jnp.where((block_of(source) == one_side) | (block_of(source) == far), factor * values, values)


def level_of(stream_key, shape, pieces, low, top_value):
    level, own = 1.0, jax.random.fold_in(stream_key, 6)
    for axis_at, parts in pieces:
        steps = jnp.exp(jax.random.uniform(jax.random.fold_in(own, axis_at), (parts,), jnp.float32, low / len(pieces), top_value / len(pieces)))
        level = level * jnp.repeat(steps, shape[axis_at] // parts).reshape([-1 if axis == axis_at else 1 for axis in range(len(shape))])
    return level


def gaussian(own_key, shape, deviation, limit, shards=(), kind=jnp.bfloat16):
    result = jax.random.normal(own_key, shape, jnp.float32) * deviation
    if len(shards) > 0:
        result = level_of(own_key, shape, shards, -0.22, 0.18) * result
    return jnp.clip(result, min=-limit, max=limit).astype(kind)


def noise_with(key, shape, deviation, reach, split, heavy, kind=jnp.bfloat16):
    values = deviation * jax.random.normal(key, shape, jnp.float32)
    if split:
        values = values * level_of(key, shape, split, -0.22, 0.18)
    return jnp.clip(spiked(values, jax.random.fold_in(key, 3), *heavy), -reach, reach).astype(kind)


def setup_inputs(seed: int = 0) -> dict:
    seeds = jax.random.split(jax.random.key(seed), 5)
    return {
        "amplitudes": gaussian(seeds[0], (IJ, K), 1.0, 6.0, ((0, 4), (1, 8)), jnp.float32),
        "integrals": noise_with(seeds[1], (K, AB), K ** -0.5, 0.03125, ((0, 8), (1, 4)), (0, 1, 8, 2.0), jnp.float32),
        "occ_energy": jnp.clip(jax.random.uniform(seeds[2], (NO,), jnp.float32, -2.0, -0.5), -2.0, -0.5),
        "vir_energy": jnp.clip(jax.random.uniform(seeds[3], (NV,), jnp.float32, 0.2, 3.0), 0.2, 3.0),
    }


def reference(amplitudes, integrals, occ_energy, vir_energy):
    first_np, second_np = np.triu_indices(NO, 1)
    first_index = jnp.asarray(first_np, dtype=jnp.int32)
    second_index = jnp.asarray(second_np, dtype=jnp.int32)
    ladder = jnp.dot(amplitudes, integrals, precision=lax.Precision.HIGHEST, preferred_element_type=jnp.float32)
    pair_sum = occ_energy[first_index] + occ_energy[second_index]
    ab_index = jnp.arange(AB, dtype=jnp.int32)
    vir_sum = vir_energy[ab_index // NV] + vir_energy[ab_index % NV]
    denominator = pair_sum[:, None] - vir_sum[None, :]
    return ladder, ladder / denominator
```

```python
import functools

import jax
import jax.numpy as jnp
import numpy as np
from jax import lax
from jax.experimental import pallas as pl
from jax.experimental.pallas import tpu as pltpu
from jax.sharding import PartitionSpec as P

MESH = pl.DeviceIdType.MESH
CHUNK = 384
PIECE = 16
LAG = 4


def lookup(indices, values_table):
    positions = jnp.arange(values_table.shape[0], dtype=jnp.int32)
    picked = jnp.where(indices[:, None] == positions[None, :], values_table[None, :], 0.0)
    return jnp.sum(picked, axis=1)


def owner_blocks(partial_sum):
    col_count = lax.axis_size("col")
    layer_count = lax.axis_size("layer")
    pair_rows = partial_sum.shape[0] // col_count
    slab_cols = partial_sum.shape[1] // layer_count
    blocks = partial_sum.reshape(col_count, pair_rows, layer_count, slab_cols)
    return blocks.transpose(0, 2, 1, 3).reshape(col_count * layer_count * pair_rows, slab_cols)


def split(value):
    high = value.astype(jnp.bfloat16)
    return high, (value - high.astype(jnp.float32)).astype(jnp.bfloat16)


def product(columns, rows):
    dims = (((1,), (1,)), ((), ()))

    def dot(left, right):
        return lax.dot_general(left, right, dims, preferred_element_type=jnp.float32)

    column_high, column_low = columns
    row_high, row_low = rows
    return (
        dot(column_low, row_high) + dot(column_high, row_low) + dot(column_high, row_high)
    )


def line_kernel(
    pair_rows,
    near,
    t_hbm,
    tail_hbm,
    v_hbm,
    out,
    rows,
    lent,
    land,
    acc,
    from_core,
    from_x,
    from_y,
    owned,
    load_sem,
    whole_sem,
    third_sem,
    lent_sem,
    sent_sem,
    hop_send,
    hop_recv,
    home_send,
    home_recv,
):
    chunks = land.shape[1]
    far = chunks - near
    thirds = acc.shape[1]
    group_rows = acc.shape[2]
    half_rows = group_rows // 2
    row = lax.axis_index("row")
    col = lax.axis_index("col")
    layer = lax.axis_index("layer")
    core = layer % 2
    x_side = layer // 2
    half = row // 2
    edge = (row == 0) | (row == 3)
    home = col == half
    edge_row = 3 * half
    inner_row = 1 + half
    far_inner = 2 - half
    far_edge = 3 - 3 * half
    core_mate = {"layer": x_side * 2 + (1 - core)}
    x_mate = {"layer": (1 - x_side) * 2 + core}
    y_mate = {"col": 1 - col}

    def remote(source, target, send_sem, recv_sem, device):
        return pltpu.make_async_remote_copy(
            src_ref=source,
            dst_ref=target,
            send_sem=send_sem,
            recv_sem=recv_sem,
            device_id=device,
            device_id_type=MESH,
        )

    def arrived(target, sem):
        pltpu.make_async_copy(target, target, sem).wait()

    def third_rows(third):
        return pl.ds(pl.multiple_of(third * group_rows, group_rows), group_rows)

    owned[...] = jnp.zeros_like(owned)
    barrier = pltpu.get_barrier_semaphore()
    for step in range(1, 4):
        pl.semaphore_signal(
            barrier, inc=1, device_id={"row": (row + step) % 4}, device_id_type=MESH
        )
    for mate in (core_mate, x_mate, y_mate):
        pl.semaphore_signal(barrier, inc=1, device_id=mate, device_id_type=MESH)
    rows_real = pl.ds(0, pair_rows)
    pl.semaphore_wait(barrier, 6)

    @pl.when(edge)
    def _():
        def send_far(i, carry):
            c = near + i
            remote(
                v_hbm.at[c], land.at[1, c], sent_sem.at[0], whole_sem.at[1, c],
                {"row": inner_row},
            ).start()
            return carry

        def send_lent(c, carry):
            start = pl.multiple_of(c * CHUNK, CHUNK)
            remote(
                t_hbm.at[:, pl.ds(start, CHUNK)], lent.at[c, rows_real], sent_sem.at[1],
                lent_sem.at[c], {"row": inner_row},
            ).start()
            return carry

        def send_near(n, carry):
            third, c = n // near, n % near
            remote(
                v_hbm.at[c, third_rows(third)], land.at[1, c, third_rows(third)],
                sent_sem.at[2], third_sem.at[0, n], {"row": inner_row},
            ).start()
            return carry

        lax.fori_loop(0, far, send_far, 0)
        lax.fori_loop(0, near, send_lent, 0)
        lax.fori_loop(0, near * thirds, send_near, 0)

    @pl.when(jnp.logical_not(edge))
    def _():
        def send_far(i, carry):
            c = near + i
            remote(
                v_hbm.at[c], land.at[2, c], sent_sem.at[0], whole_sem.at[2, c],
                {"row": far_inner},
            ).start()
            remote(
                v_hbm.at[c], land.at[1, c], sent_sem.at[1], whole_sem.at[1, c],
                {"row": edge_row},
            ).start()
            return carry

        def send_near(c, carry):
            remote(
                v_hbm.at[c], land.at[2, c], sent_sem.at[2], whole_sem.at[2, c],
                {"row": far_inner},
            ).start()
            return carry

        lax.fori_loop(0, far, send_far, 0)
        lax.fori_loop(0, near, send_near, 0)

    pltpu.make_async_copy(v_hbm, land.at[0], load_sem.at[0]).start()

    def load_rows(c, carry):
        start = pl.multiple_of(c * CHUNK, CHUNK)
        pltpu.make_async_copy(
            t_hbm.at[:, pl.ds(start, CHUNK)], rows.at[c, rows_real], load_sem.at[1]
        ).start()
        return carry

    lax.fori_loop(0, chunks - 1, load_rows, 0)
    pltpu.make_async_copy(
        tail_hbm, rows.at[chunks - 1, rows_real], load_sem.at[1]
    ).start()
    acc[...] = jnp.zeros_like(acc)
    spare = pl.ds(pair_rows, rows.shape[1] - pair_rows)

    def clear_rows(c, carry):
        rows[c, spare] = jnp.zeros_like(rows[c, spare])
        return carry

    def clear_lent(c, carry):
        lent[c, spare] = jnp.zeros_like(lent[c, spare])
        return carry

    lax.fori_loop(0, chunks, clear_rows, 0)
    lax.fori_loop(0, near, clear_lent, 0)
    arrived(land.at[0], load_sem.at[0])
    arrived(rows.at[:, rows_real], load_sem.at[1])

    def add_whole(block, c, pairs):
        other = split(block[c])
        for slot, part in pairs:
            sums = product(split(land[part, c]), other)
            acc[slot] += sums.reshape(acc.shape[1:])

    def add_third(block, c, third, pairs):
        other = split(block[c])
        for slot, part in pairs:
            acc[slot, third] += product(split(land[part, c, third_rows(third)]), other)

    half_mine = pl.ds(pl.multiple_of(core * half_rows, half_rows), half_rows)
    half_given = pl.ds(pl.multiple_of((1 - core) * half_rows, half_rows), half_rows)
    mine = pl.ds(pl.multiple_of(core * half_rows + x_side * PIECE, PIECE), PIECE)
    x_given = pl.ds(pl.multiple_of(core * half_rows + (1 - x_side) * PIECE, PIECE), PIECE)

    class Unit:
        def __init__(self, index, slots, group):
            self.index, self.slots, self.group = index, slots, group

        def core_copy(self):
            return remote(
                acc.at[self.slots, self.group, half_given],
                from_core.at[self.slots, self.group],
                hop_send.at[self.index, 0], hop_recv.at[self.index, 0], core_mate,
            )

        def x_copy(self):
            return remote(
                acc.at[self.slots, self.group, x_given],
                from_x.at[self.slots, self.group],
                hop_send.at[self.index, 1], hop_recv.at[self.index, 1], x_mate,
            )

        def y_copy(self):
            return remote(
                acc.at[self.slots, self.group, mine],
                from_y.at[self.slots, self.group],
                hop_send.at[self.index, 2], hop_recv.at[self.index, 2], y_mate,
            )

        def start(self):
            self.core_copy().start()

        def second(self):
            self.core_copy().wait()
            acc[self.slots, self.group, half_mine] += from_core[self.slots, self.group]
            self.x_copy().start()

        def third(self):
            self.x_copy().wait()
            acc[self.slots, self.group, mine] += from_x[self.slots, self.group]

            @pl.when(jnp.logical_not(home))
            def _():
                self.y_copy().start()

        def last(self, targets):
            @pl.when(jnp.logical_not(home))
            def _():
                self.y_copy().wait_send()

            @pl.when(home)
            def _():
                self.y_copy().wait_recv()
                acc[self.slots, self.group, mine] += from_y[self.slots, self.group]
                for slot, kind, device, send, recv in targets:
                    if device is None:
                        owned[kind, self.group] = acc[slot, self.group, mine]
                    else:
                        remote(
                            acc.at[slot, self.group, mine], owned.at[kind, self.group],
                            home_send.at[send], home_recv.at[recv], {"row": device},
                        ).start()

        def run(self, targets):
            self.start()
            self.second()
            self.third()
            self.last(targets)

    every = pl.ds(0, thirds)

    def kind_sem(kind, group):
        return kind * thirds + group

    @pl.when(edge)
    def _():
        def own(c, carry):
            add_whole(rows, c, ((0, 0),))
            return carry

        def other(part, i, carry):
            c = near + i
            arrived(land.at[part, c], whole_sem.at[part, c])
            add_whole(rows, c, ((part, part),))
            return carry

        lax.fori_loop(0, chunks, own, 0)
        lax.fori_loop(0, far, functools.partial(other, 1), 0)
        Unit(0, pl.ds(0, 2), every).run(
            ((0, 0, None, 0, 0), (1, 0, inner_row, 0, kind_sem(0, 0)))
        )
        lax.fori_loop(0, far, functools.partial(other, 2), 0)
        Unit(1, pl.ds(2, 1), every).run(((2, 0, far_inner, 1, kind_sem(0, 0)),))
        lax.fori_loop(0, far, functools.partial(other, 3), 0)
        Unit(2, pl.ds(3, 1), every).run(((3, 0, far_edge, 2, kind_sem(0, 0)),))

        @pl.when(home)
        def _():
            for send, slot in ((0, 1), (1, 2), (2, 3)):
                remote(
                    acc.at[slot, every, mine], owned.at[0, every],
                    home_send.at[send], home_recv.at[0], {"row": inner_row},
                ).wait_send()

        arrived_far = pl.ds(near, far)
        for at, source in (
            (0, land.at[0, arrived_far]), (2, land.at[0, pl.ds(0, near)]),
        ):
            remote(
                source, source, sent_sem.at[at], whole_sem.at[0, 0], {"row": inner_row}
            ).wait_send()
        remote(
            rows.at[pl.ds(0, near), rows_real], rows.at[pl.ds(0, near), rows_real],
            sent_sem.at[1], whole_sem.at[0, 0], {"row": inner_row},
        ).wait_send()

    @pl.when(jnp.logical_not(edge))
    def _():
        def first_far(i, carry):
            c = near + i
            arrived(land.at[1, c], whole_sem.at[1, c])
            remote(
                land.at[1, c], land.at[3, c], sent_sem.at[3], whole_sem.at[3, c],
                {"row": far_inner},
            ).start()
            arrived(land.at[2, c], whole_sem.at[2, c])
            remote(
                land.at[2, c], land.at[2, c], sent_sem.at[4], whole_sem.at[2, c],
                {"row": edge_row},
            ).start()
            add_whole(rows, c, ((0, 0), (4, 1), (1, 2)))
            return carry

        def first_near(c, carry):
            arrived(land.at[2, c], whole_sem.at[2, c])
            add_whole(rows, c, ((0, 0), (1, 2)))
            return carry

        def lent_chunk(c, carry):
            arrived(lent.at[c, rows_real], lent_sem.at[c])
            add_whole(lent, c, ((2, 0), (3, 2)))
            return carry

        def second_far(i, carry):
            c = near + i
            arrived(land.at[3, c], whole_sem.at[3, c])
            remote(
                land.at[3, c], land.at[3, c], sent_sem.at[5], whole_sem.at[3, c],
                {"row": edge_row},
            ).start()
            add_whole(rows, c, ((5, 3),))
            return carry

        lax.fori_loop(0, far, first_far, 0)
        early = near // 3

        def early_block(m, carry):
            lax.fori_loop(3 * m, 3 * m + 3, first_near, 0)
            return lent_chunk(m, carry)

        lax.fori_loop(0, early, early_block, 0)
        Unit(0, pl.ds(0, 2), every).run(
            ((0, 1, None, 0, 0), (1, 1, far_inner, 0, kind_sem(1, 0)))
        )
        late = near - early
        per = far // (late - 1)

        def late_block(m, carry):
            lax.fori_loop(per * m, per * m + per, second_far, 0)
            return lent_chunk(early + m, carry)

        lax.fori_loop(0, late - 1, late_block, 0)
        lax.fori_loop(per * (late - 1), far, second_far, 0)
        lent_chunk(near - 1, 0)

        lent_unit = Unit(1, pl.ds(2, 2), every)
        lent_targets = ((2, 2, None, 0, 0), (3, 2, far_inner, 1, kind_sem(2, 0)))

        def third_unit(third):
            return Unit(2 + third, pl.ds(4, 3), third)

        def third_targets(third):
            return (
                (4, 1, edge_row, 2 + third, kind_sem(1, third)),
                (5, 1, far_edge, 2 + thirds + third, kind_sem(1, third)),
                (6, 2, far_edge, 2 + 2 * thirds + third, kind_sem(2, third)),
            )

        pieces = near * thirds

        def pass_on(n):
            third, c = n // near, n % near
            arrived(land.at[1, c, third_rows(third)], third_sem.at[0, n])
            remote(
                land.at[1, c, third_rows(third)], land.at[3, c, third_rows(third)],
                sent_sem.at[6], third_sem.at[1, n], {"row": far_inner},
            ).start()

        def near_step(n, carry):
            third, c = n // near, n % near
            ahead = n + LAG

            @pl.when(ahead < pieces)
            def _():
                pass_on(ahead)

            add_third(rows, c, third, ((4, 1),))
            arrived(land.at[3, c, third_rows(third)], third_sem.at[1, n])
            add_third(rows, c, third, ((5, 3),))
            add_third(lent, c, third, ((6, 3),))

            first = third == 0
            before = third - 1

            def staged(at, on_lent, on_third):
                pl.when((c == at) & first)(on_lent)
                pl.when((c == at) & jnp.logical_not(first))(on_third)

            staged(1, lent_unit.start, lambda: third_unit(before).start())
            staged(3, lent_unit.second, lambda: third_unit(before).second())
            staged(5, lent_unit.third, lambda: third_unit(before).third())
            staged(
                7,
                lambda: lent_unit.last(lent_targets),
                lambda: third_unit(before).last(third_targets(before)),
            )
            return carry

        for n in range(LAG):
            pass_on(n)
        lax.fori_loop(0, pieces, near_step, 0)
        third_unit(thirds - 1).run(third_targets(thirds - 1))

        @pl.when(home)
        def _():
            sends = [(0, 1, every), (1, 3, every)]
            for at, slot in enumerate((4, 5, 6)):
                sends += [(2 + at * thirds + k, slot, k) for k in range(thirds)]
            for send, slot, group in sends:
                remote(
                    acc.at[slot, group, mine], owned.at[1, group],
                    home_send.at[send], home_recv.at[0], {"row": far_inner},
                ).wait_send()

        arrived_far = pl.ds(near, far)
        arrived_near = pl.ds(0, near)
        for at, source in (
            (0, land.at[0, arrived_far]),
            (1, land.at[0, arrived_far]),
            (2, land.at[0, arrived_near]),
            (3, land.at[1, arrived_far]),
            (4, land.at[2, arrived_far]),
            (5, land.at[3, arrived_far]),
            (6, land.at[1, arrived_near]),
        ):
            remote(
                source, source, sent_sem.at[at], whole_sem.at[0, 0], {"row": far_inner}
            ).wait_send()

    def owned_whole(kind):
        arrived(owned.at[kind, every], home_recv.at[kind_sem(kind, 0)])

    def owned_thirds(kind):
        for third in range(thirds):
            arrived(owned.at[kind, third], home_recv.at[kind_sem(kind, third)])

    @pl.when(edge & home)
    def _():
        owned_thirds(1)

    @pl.when(jnp.logical_not(edge) & home)
    def _():
        owned_whole(0)

    @pl.when(edge & jnp.logical_not(home))
    def _():
        owned_whole(0)
        owned_thirds(1)
        owned_thirds(2)

    @pl.when(jnp.logical_not(edge) & jnp.logical_not(home))
    def _():
        owned_whole(0)
        owned_whole(1)
        owned_whole(2)

    out[col] = owned[0] + owned[2]
    out[1 - col] = owned[1]


def line_exchange(amplitudes, integrals):
    pair_rows = amplitudes.shape[0]
    depth, width = integrals.shape
    chunks = -(-depth // CHUNK)
    near = 3 * chunks // 8
    layers = lax.axis_size("layer")
    thirds = width // (layers * PIECE)
    padded = -(-pair_rows // 128) * 128
    tail = jnp.pad(
        amplitudes[:, (chunks - 1) * CHUNK :], ((0, 0), (0, chunks * CHUNK - depth))
    )
    columns = jnp.pad(integrals, ((0, chunks * CHUNK - depth), (0, 0)))
    columns = columns.reshape(chunks, CHUNK, layers // 2, 2, thirds, PIECE)
    columns = columns.transpose(0, 4, 3, 2, 5, 1).reshape(chunks, width, CHUNK)
    group = width // thirds
    vmem = functools.partial(pltpu.VMEM, dtype=jnp.float32)
    dma = pltpu.SemaphoreType.DMA
    flops = 2 * 3 * 5 * pair_rows * depth * width
    out = pl.pallas_call(
        functools.partial(line_kernel, pair_rows, near),
        out_shape=jax.ShapeDtypeStruct((2, thirds, PIECE, padded), jnp.float32),
        in_specs=[pl.BlockSpec(memory_space=pl.ANY)] * 3,
        out_specs=pl.BlockSpec(memory_space=pltpu.VMEM),
        scratch_shapes=[
            vmem((chunks, padded, CHUNK)),
            vmem((near, padded, CHUNK)),
            vmem((4, chunks, width, CHUNK)),
            vmem((7, thirds, group, padded)),
            vmem((7, thirds, group // 2, padded)),
            vmem((7, thirds, PIECE, padded)),
            vmem((7, thirds, PIECE, padded)),
            vmem((3, thirds, PIECE, padded)),
            dma((2,)),
            dma((4, chunks)),
            dma((2, near * thirds)),
            dma((near,)),
            dma((7,)),
            dma((2 + thirds, 3)),
            dma((2 + thirds, 3)),
            dma((2 + 3 * thirds,)),
            dma((3 * thirds,)),
        ],
        compiler_params=pltpu.CompilerParams(
            collective_id=0, has_side_effects=True, vmem_limit_bytes=67043328
        ),
        cost_estimate=pl.CostEstimate(
            flops=flops, bytes_accessed=4 * depth * (pair_rows + width), transcendentals=0
        ),
    )(amplitudes, tail, columns)
    blocks = out.reshape(2, thirds * PIECE, padded)[:, :, :pair_rows]
    return blocks.transpose(0, 2, 1).reshape(2 * pair_rows, thirds * PIECE)


def gathered(amplitudes, integrals):
    partial_rows = jnp.dot(
        amplitudes,
        lax.all_gather(integrals, "row", axis=1, tiled=True),
        precision=lax.Precision.HIGHEST,
        preferred_element_type=jnp.float32,
    )
    partial_sum = lax.all_to_all(partial_rows, "row", split_axis=1, concat_axis=0, tiled=True)
    return lax.psum_scatter(
        owner_blocks(partial_sum), ("col", "layer"), scatter_dimension=0, tiled=True
    )


def fits_line(amplitudes, integrals):
    pair_rows = amplitudes.shape[0]
    depth, width = integrals.shape
    chunks = -(-depth // CHUNK)
    near = 3 * chunks // 8
    split_evenly = width % (4 * PIECE) == 0 and pair_rows % 8 == 0 and near % 3 == 0
    words = chunks * (4 * width + pair_rows) + near * pair_rows
    return split_evenly and near >= 9 and words * CHUNK * 4 < 56 * 2**20


def shards(amplitudes, integrals, occ_energy, vir_energy):
    in_line = lax.axis_size("row") == 4 and lax.axis_size("col") == 2
    in_line = in_line and lax.axis_size("layer") == 4
    if in_line and fits_line(amplitudes, integrals):
        ladder = line_exchange(amplitudes, integrals)
    else:
        ladder = gathered(amplitudes, integrals)
    pair_rows = ladder.shape[0]
    slab_cols = ladder.shape[1]
    occupied = occ_energy.shape[0]
    virtuals = vir_energy.shape[0]
    first_np, second_np = np.triu_indices(occupied, 1)
    ij_start = lax.axis_index("col") * pair_rows
    ab_start = (
        lax.axis_index("row") * lax.axis_size("layer") + lax.axis_index("layer")
    ) * slab_cols
    first_index = lax.dynamic_slice_in_dim(
        jnp.asarray(first_np, dtype=jnp.int32), ij_start, pair_rows
    )
    second_index = lax.dynamic_slice_in_dim(
        jnp.asarray(second_np, dtype=jnp.int32), ij_start, pair_rows
    )
    pair_sum = lookup(first_index, occ_energy) + lookup(second_index, occ_energy)
    ab_index = ab_start + jnp.arange(slab_cols, dtype=jnp.int32)
    vir_sum = lookup(ab_index // virtuals, vir_energy) + lookup(ab_index % virtuals, vir_energy)
    denominator = pair_sum[:, None] - vir_sum[None, :]
    return (ladder, ladder / denominator)


def solution(mesh):
    in_specs = (P("row", ("layer", "col")), P(("layer", "col"), "row"), P(), P())
    out_specs = (P("col", ("row", "layer")), P("col", ("row", "layer")))
    return jax.shard_map(shards, mesh=mesh, in_specs=in_specs, out_specs=out_specs, check_vma=False)
```

```python
import functools

import jax
import jax.numpy as jnp
import numpy as np
from jax import lax
from jax.experimental import pallas as pl
from jax.experimental.pallas import tpu as pltpu
from jax.sharding import PartitionSpec as P

MESH = pl.DeviceIdType.MESH
CHUNK = 384
PIECE = 16
LAG = 4
STAGES = 4


def lookup(indices, values_table):
    positions = jnp.arange(values_table.shape[0], dtype=jnp.int32)
    picked = jnp.where(indices[:, None] == positions[None, :], values_table[None, :], 0.0)
    return jnp.sum(picked, axis=1)


def owner_blocks(partial_sum):
    col_count = lax.axis_size("col")
    layer_count = lax.axis_size("layer")
    pair_rows = partial_sum.shape[0] // col_count
    slab_cols = partial_sum.shape[1] // layer_count
    blocks = partial_sum.reshape(col_count, pair_rows, layer_count, slab_cols)
    return blocks.transpose(0, 2, 1, 3).reshape(col_count * layer_count * pair_rows, slab_cols)


def split(value):
    high = value.astype(jnp.bfloat16)
    return high, (value - high.astype(jnp.float32)).astype(jnp.bfloat16)


def product(columns, rows):
    dims = (((1,), (1,)), ((), ()))

    def dot(left, right):
        return lax.dot_general(left, right, dims, preferred_element_type=jnp.float32)

    column_high, column_low = columns
    row_high, row_low = rows
    return (
        dot(column_low, row_high) + dot(column_high, row_low) + dot(column_high, row_high)
    )


def denominators(pair_rows, occ, vir, below):
    row = lax.axis_index("row")
    col = lax.axis_index("col")
    layer = lax.axis_index("layer")
    blocks, slab, lanes = below.shape
    occupied = occ.shape[0]
    virtuals = vir.shape[0]
    shape = (8, lanes)
    block = lax.broadcasted_iota(jnp.int32, shape, 0)
    pair = (blocks * col + block) * pair_rows + lax.broadcasted_iota(jnp.int32, shape, 1)

    def begin(k):
        return k * (2 * occupied - k - 1) // 2

    def pick_first(k, carry):
        energy, second = carry
        inside = (pair >= begin(k)) & (pair < begin(k + 1))
        return (
            energy + jnp.where(inside, occ[k], 0.0),
            jnp.where(inside, pair - begin(k) + k + 1, second),
        )

    zeros = jnp.zeros(shape, jnp.float32)
    first_energy, second = lax.fori_loop(
        0, occupied, pick_first, (zeros, jnp.zeros(shape, jnp.int32))
    )

    def pick_second(k, energy):
        return energy + jnp.where(second == k, occ[k], 0.0)

    pair_sum = first_energy + lax.fori_loop(0, occupied, pick_second, zeros)
    start = (row * lax.axis_size("layer") + layer) * slab

    def fill(i, carry):
        index = start + i
        vir_sum = jnp.full(shape, vir[index // virtuals]) + vir[index % virtuals]
        value = pair_sum - vir_sum
        for at in range(blocks):
            below[at, pl.ds(i, 1)] = value[at : at + 1]
        return carry

    lax.fori_loop(0, slab, fill, 0)


def line_kernel(
    near,
    t_hbm,
    v_hbm,
    occ_hbm,
    vir_hbm,
    out,
    step_out,
    rows,
    lent,
    land,
    acc,
    from_core,
    from_x,
    from_y,
    owned,
    relay,
    stage,
    below,
    tail,
    occ,
    vir,
    load_sem,
    stage_sem,
    whole_sem,
    third_sem,
    lent_sem,
    sent_sem,
    hop_send,
    hop_recv,
    home_send,
    home_recv,
    relay_recv,
):
    pair_rows, depth = t_hbm.shape
    chunks = land.shape[1]
    far = chunks - near
    thirds = acc.shape[1]
    group_rows = acc.shape[2]
    half_rows = group_rows // 2
    row = lax.axis_index("row")
    col = lax.axis_index("col")
    layer = lax.axis_index("layer")
    core = layer % 2
    x_side = layer // 2
    half = row // 2
    edge = (row == 0) | (row == 3)
    home = col == half
    edge_row = 3 * half
    inner_row = 1 + half
    far_inner = 2 - half
    far_edge = 3 - 3 * half
    core_mate = {"layer": x_side * 2 + (1 - core)}
    x_mate = {"layer": (1 - x_side) * 2 + core}
    y_mate = {"col": 1 - col}

    def remote(source, target, send_sem, recv_sem, device):
        return pltpu.make_async_remote_copy(
            src_ref=source,
            dst_ref=target,
            send_sem=send_sem,
            recv_sem=recv_sem,
            device_id=device,
            device_id_type=MESH,
        )

    def arrived(target, sem):
        pltpu.make_async_copy(target, target, sem).wait()

    def third_rows(third):
        return pl.ds(pl.multiple_of(third * group_rows, group_rows), group_rows)

    last_start = (chunks - 1) * CHUNK
    last_depth = depth - last_start
    rows_real = pl.ds(0, pair_rows)
    spare = pl.ds(pair_rows, rows.shape[1] - pair_rows)

    def chunk_at(j):
        return jnp.where(j < far - 1, near + j, j - (far - 1))

    def stage_copy(j):
        start = pl.multiple_of(chunk_at(j) * CHUNK, CHUNK)
        slot = j % STAGES
        return pltpu.make_async_copy(
            v_hbm.at[pl.ds(start, CHUNK)], stage.at[slot], stage_sem.at[slot]
        )

    last_stage = pltpu.make_async_copy(
        v_hbm.at[pl.ds(last_start, last_depth)],
        stage.at[STAGES, pl.ds(0, last_depth)],
        stage_sem.at[STAGES],
    )

    def load_rows(c):
        start = pl.multiple_of(c * CHUNK, CHUNK)
        pltpu.make_async_copy(
            t_hbm.at[:, pl.ds(start, CHUNK)], rows.at[c, rows_real], load_sem.at[0]
        ).start()

    barrier = pltpu.get_barrier_semaphore()
    owned[...] = jnp.zeros_like(owned)
    for step in range(1, 4):
        pl.semaphore_signal(
            barrier, inc=1, device_id={"row": (row + step) % 4}, device_id_type=MESH
        )
    for mate in (core_mate, x_mate, y_mate):
        pl.semaphore_signal(barrier, inc=1, device_id=mate, device_id_type=MESH)
    for j in range(STAGES):
        stage_copy(j).start()
    if last_depth < CHUNK:
        lost = pl.ds(last_depth, CHUNK - last_depth)
        stage[STAGES, lost] = jnp.zeros_like(stage[STAGES, lost])
        rows[chunks - 1] = jnp.zeros_like(rows[chunks - 1])
    last_stage.start()
    last_rows = (
        t_hbm.at[:, pl.ds(last_start, last_depth)],
        tail,
        load_sem.at[1],
    )
    slab = thirds * PIECE

    def turn(slot, c):
        turned = stage[slot].T
        for third in range(thirds):
            for at_core in range(2):
                for at_x in range(2):
                    source = (at_x * 2 + at_core) * slab + third * PIECE
                    target = third * group_rows + at_core * half_rows + at_x * PIECE
                    land[0, c, pl.ds(target, PIECE)] = turned[source : source + PIECE]

    def prepare(j):
        c = chunk_at(j)
        stage_copy(j).wait()
        turn(j % STAGES, c)

        @pl.when(j + STAGES < chunks - 1)
        def _():
            stage_copy(j + STAGES).start()

        load_rows(c)

    def send_far(c):
        @pl.when(edge)
        def _():
            remote(
                land.at[0, c], land.at[1, c], sent_sem.at[0], whole_sem.at[1, c],
                {"row": inner_row},
            ).start()

        @pl.when(jnp.logical_not(edge))
        def _():
            remote(
                land.at[0, c], land.at[2, c], sent_sem.at[0], whole_sem.at[2, c],
                {"row": far_inner},
            ).start()
            remote(
                land.at[0, c], land.at[1, c], sent_sem.at[1], whole_sem.at[1, c],
                {"row": edge_row},
            ).start()

    def send_near(c):
        remote(
            land.at[0, c], land.at[2, c], sent_sem.at[2], whole_sem.at[2, c],
            {"row": far_inner},
        ).start()

    prepare(0)
    pl.semaphore_wait(barrier, 6)

    def far_loop(j, carry):
        prepare(j)
        send_far(near + j - 1)
        return carry

    lax.fori_loop(1, far - 1, far_loop, 0)
    last_stage.wait()
    turn(STAGES, chunks - 1)
    send_far(chunks - 2)
    pltpu.make_async_copy(*last_rows).start()
    prepare(far - 1)
    send_far(chunks - 1)

    @pl.when(edge)
    def _():
        def send_lent(c, carry):
            start = pl.multiple_of(c * CHUNK, CHUNK)
            remote(
                t_hbm.at[:, pl.ds(start, CHUNK)], lent.at[c, rows_real], sent_sem.at[1],
                lent_sem.at[c], {"row": inner_row},
            ).start()
            return carry

        lax.fori_loop(0, near, send_lent, 0)

    def near_loop(c, carry):
        prepare(far - 1 + c)
        pl.when(jnp.logical_not(edge))(lambda: send_near(c - 1))
        return carry

    lax.fori_loop(1, near, near_loop, 0)
    acc[...] = jnp.zeros_like(acc)

    @pl.when(edge)
    def _():
        def send_piece(n, carry):
            third, c = n // near, n % near
            remote(
                land.at[0, c, third_rows(third)], land.at[1, c, third_rows(third)],
                sent_sem.at[2], third_sem.at[0, n], {"row": inner_row},
            ).start()
            return carry

        lax.fori_loop(0, near * thirds, send_piece, 0)

    pl.when(jnp.logical_not(edge))(lambda: send_near(near - 1))
    energies = (
        pltpu.make_async_copy(occ_hbm, occ, load_sem.at[2]),
        pltpu.make_async_copy(vir_hbm, vir, load_sem.at[3]),
    )
    for copy in energies:
        copy.start()

    def clear_rows(c, carry):
        rows[c, spare] = jnp.zeros_like(rows[c, spare])
        return carry

    def clear_lent(c, carry):
        lent[c, spare] = jnp.zeros_like(lent[c, spare])
        return carry

    lax.fori_loop(0, chunks - 1, clear_rows, 0)
    lax.fori_loop(0, near, clear_lent, 0)
    for copy in energies:
        copy.wait()
    denominators(pair_rows, occ, vir, below)
    arrived(rows.at[pl.ds(0, chunks - 1), rows_real], load_sem.at[0])
    pltpu.make_async_copy(*last_rows).wait()
    rows[chunks - 1, rows_real, pl.ds(0, last_depth)] = tail[...]

    def add_whole(block, c, pairs):
        other = split(block[c])
        for slot, part in pairs:
            sums = product(split(land[part, c]), other)
            acc[slot] += sums.reshape(acc.shape[1:])

    def add_third(block, c, third, pairs):
        other = split(block[c])
        for slot, part in pairs:
            acc[slot, third] += product(split(land[part, c, third_rows(third)]), other)

    half_mine = pl.ds(pl.multiple_of(core * half_rows, half_rows), half_rows)
    half_given = pl.ds(pl.multiple_of((1 - core) * half_rows, half_rows), half_rows)
    mine = pl.ds(pl.multiple_of(core * half_rows + x_side * PIECE, PIECE), PIECE)
    x_given = pl.ds(pl.multiple_of(core * half_rows + (1 - x_side) * PIECE, PIECE), PIECE)

    class Unit:
        def __init__(self, index, slots, group, here, there):
            self.index, self.slots, self.group = index, slots, group
            self.here, self.there = here, there
            self.slot_here, self.slot_there = here is not None, there is not None
            if self.slot_here and self.slot_there:
                self.kept = jnp.where(home, here, there)
                self.given = jnp.where(home, there, here)
                self.gives = self.takes = True
            else:
                self.kept = self.given = slots
                self.takes = home if self.slot_here else jnp.logical_not(home)
                self.gives = jnp.logical_not(self.takes)

        def core_copy(self):
            return remote(
                acc.at[self.slots, self.group, half_given],
                from_core.at[self.slots, self.group],
                hop_send.at[self.index, 0], hop_recv.at[self.index, 0], core_mate,
            )

        def x_copy(self):
            return remote(
                acc.at[self.slots, self.group, x_given],
                from_x.at[self.slots, self.group],
                hop_send.at[self.index, 1], hop_recv.at[self.index, 1], x_mate,
            )

        def y_copy(self):
            return remote(
                acc.at[self.given, self.group, mine],
                from_y.at[self.given, self.group],
                hop_send.at[self.index, 2], hop_recv.at[self.index, 2], y_mate,
            )

        def start(self):
            self.core_copy().start()

        def second(self):
            self.core_copy().wait()
            acc[self.slots, self.group, half_mine] += from_core[self.slots, self.group]
            self.x_copy().start()

        def third(self):
            self.x_copy().wait()
            acc[self.slots, self.group, mine] += from_x[self.slots, self.group]
            when(self.gives, lambda: self.y_copy().start())

        def last(self, targets_here, targets_there=()):
            when(self.gives, lambda: self.y_copy().wait_send())

            def take():
                self.y_copy().wait_recv()
                acc[self.kept, self.group, mine] += from_y[self.kept, self.group]

            when(self.takes, take)

            def deliver(targets):
                for slot, target, device, send, recv in targets:
                    source = acc.at[slot, self.group, mine]
                    if device is None:
                        target[self.group] = source[...]
                    else:
                        remote(
                            source, target.at[self.group], home_send.at[send], recv,
                            {"row": device},
                        ).start()

            if targets_here:
                pl.when(home)(lambda: deliver(targets_here))
            if targets_there:
                pl.when(jnp.logical_not(home))(lambda: deliver(targets_there))

        def run(self, targets_here, targets_there=()):
            self.start()
            self.second()
            self.third()
            self.last(targets_here, targets_there)

    def when(condition, action):
        if condition is True:
            action()
        else:
            pl.when(condition)(action)

    every = pl.ds(0, thirds)

    def kind_sem(kind, group):
        return home_recv.at[kind * thirds + group]

    @pl.when(edge)
    def _():
        def own(c, carry):
            add_whole(rows, c, ((0, 0),))
            return carry

        def other(part, i, carry):
            c = near + i
            arrived(land.at[part, c], whole_sem.at[part, c])
            add_whole(rows, c, ((part, part),))
            return carry

        lax.fori_loop(0, chunks, own, 0)
        lax.fori_loop(0, far, functools.partial(other, 1), 0)
        Unit(0, pl.ds(0, 2), every, 0, None).run(
            (
                (0, owned.at[0], None, 0, None),
                (1, owned.at[0], inner_row, 0, kind_sem(0, 0)),
            )
        )
        lax.fori_loop(0, far, functools.partial(other, 2), 0)
        Unit(1, pl.ds(2, 1), every, None, 2).run(
            (), ((2, relay.at[0], far_inner, 1, relay_recv.at[0]),)
        )
        lax.fori_loop(0, far, functools.partial(other, 3), 0)
        Unit(2, pl.ds(3, 1), every, 3, None).run(
            ((3, owned.at[0], far_edge, 2, kind_sem(0, 0)),)
        )

        def sent_home(send, group):
            remote(
                acc.at[0, group, mine], owned.at[0, group],
                home_send.at[send], home_recv.at[0], {"row": inner_row},
            ).wait_send()

        @pl.when(home)
        def _():
            sent_home(0, every)
            sent_home(2, every)

        @pl.when(jnp.logical_not(home))
        def _():
            sent_home(1, every)

        arrived_far = pl.ds(near, far)
        for at, source in (
            (0, land.at[0, arrived_far]), (2, land.at[0, pl.ds(0, near)]),
        ):
            remote(
                source, source, sent_sem.at[at], whole_sem.at[0, 0], {"row": inner_row}
            ).wait_send()
        remote(
            rows.at[pl.ds(0, near), rows_real], rows.at[pl.ds(0, near), rows_real],
            sent_sem.at[1], whole_sem.at[0, 0], {"row": inner_row},
        ).wait_send()

    @pl.when(jnp.logical_not(edge))
    def _():
        def first_far(i, carry):
            c = near + i
            arrived(land.at[1, c], whole_sem.at[1, c])
            remote(
                land.at[1, c], land.at[3, c], sent_sem.at[3], whole_sem.at[3, c],
                {"row": far_inner},
            ).start()
            arrived(land.at[2, c], whole_sem.at[2, c])
            remote(
                land.at[2, c], land.at[2, c], sent_sem.at[4], whole_sem.at[2, c],
                {"row": edge_row},
            ).start()
            add_whole(rows, c, ((0, 0), (4, 1), (1, 2)))
            return carry

        def first_near(c, carry):
            arrived(land.at[2, c], whole_sem.at[2, c])
            add_whole(rows, c, ((0, 0), (1, 2)))
            return carry

        def lent_chunk(c, carry):
            arrived(lent.at[c, rows_real], lent_sem.at[c])
            add_whole(lent, c, ((2, 0), (3, 2)))
            return carry

        def second_far(i, carry):
            c = near + i
            arrived(land.at[3, c], whole_sem.at[3, c])
            remote(
                land.at[3, c], land.at[3, c], sent_sem.at[5], whole_sem.at[3, c],
                {"row": edge_row},
            ).start()
            add_whole(rows, c, ((5, 3),))
            return carry

        lax.fori_loop(0, far, first_far, 0)
        early = near // 3

        def early_block(m, carry):
            lax.fori_loop(3 * m, 3 * m + 3, first_near, 0)
            return lent_chunk(m, carry)

        lax.fori_loop(0, early, early_block, 0)
        Unit(0, pl.ds(0, 2), every, 0, 1).run(
            ((0, owned.at[1], None, 0, None),),
            ((1, relay.at[1], far_inner, 0, relay_recv.at[1]),),
        )
        late = near - early
        per = far // (late - 1)

        def late_block(m, carry):
            lax.fori_loop(per * m, per * m + per, second_far, 0)
            return lent_chunk(early + m, carry)

        lax.fori_loop(0, late - 1, late_block, 0)
        lax.fori_loop(per * (late - 1), far, second_far, 0)
        lent_chunk(near - 1, 0)

        lent_unit = Unit(1, pl.ds(2, 2), every, 2, 3)
        lent_targets = (
            ((2, owned.at[2], None, 0, None),),
            ((3, relay.at[2], far_inner, 1, relay_recv.at[2]),),
        )

        def edge_unit(third):
            return Unit(2 + third, pl.ds(4, 1), third, 4, None)

        def edge_targets(third):
            return ((4, owned.at[1], edge_row, 2 + third, kind_sem(1, third)),)

        def last_unit(third):
            return Unit(2 + thirds + third, pl.ds(5, 2), third, 5, None)

        def last_targets(third):
            return (
                (5, owned.at[1], far_edge, 2 + thirds + third, kind_sem(1, third)),
                (6, owned.at[2], far_edge, 2 + 2 * thirds + third, kind_sem(2, third)),
            )

        pieces = near * thirds

        def pass_on(n):
            third, c = n // near, n % near
            arrived(land.at[1, c, third_rows(third)], third_sem.at[0, n])
            remote(
                land.at[1, c, third_rows(third)], land.at[3, c, third_rows(third)],
                sent_sem.at[6], third_sem.at[1, n], {"row": far_inner},
            ).start()
            add_third(rows, c, third, ((4, 1),))

        def near_step(n, carry):
            third, c = n // near, n % near

            @pl.when(n + LAG < pieces)
            def _():
                pass_on(n + LAG)

            arrived(land.at[3, c, third_rows(third)], third_sem.at[1, n])
            add_third(rows, c, third, ((5, 3),))
            add_third(lent, c, third, ((6, 3),))

            first = third == 0
            later = jnp.logical_not(first)
            before = third - 1
            pl.when(first & (c == 1))(lent_unit.start)
            pl.when(first & (c == 3))(lent_unit.second)
            pl.when(first & (c == 5))(lent_unit.third)
            pl.when(first & (c == 7))(lambda: lent_unit.last(*lent_targets))
            pl.when(later & (c == 1))(lambda: last_unit(before).start())
            pl.when(later & (c == 3))(lambda: last_unit(before).second())
            pl.when(later & (c == 5))(lambda: last_unit(before).third())
            pl.when(later & (c == 7))(
                lambda: last_unit(before).last(last_targets(before))
            )
            pl.when(c == near - LAG)(lambda: edge_unit(third).start())
            pl.when(c == near - LAG + 2)(lambda: edge_unit(third).second())
            pl.when(later & (c == 0))(lambda: edge_unit(before).third())
            pl.when(later & (c == 2))(
                lambda: edge_unit(before).last(edge_targets(before))
            )
            return carry

        def send_relay(kind):
            return remote(
                relay.at[kind], owned.at[kind], home_send.at[2 + 3 * thirds + kind],
                kind_sem(kind, 0), y_mate,
            )

        def relay_on(kind):
            @pl.when(home)
            def _():
                arrived(relay.at[kind], relay_recv.at[kind])
                send_relay(kind).start()

        for n in range(LAG):
            pass_on(n)
        lax.fori_loop(0, pieces, near_step, 0)
        final = thirds - 1
        last_unit(final).start()
        edge_unit(final).third()
        relay_on(1)
        last_unit(final).second()
        edge_unit(final).last(edge_targets(final))
        relay_on(2)
        last_unit(final).third()
        last_unit(final).last(last_targets(final))
        relay_on(0)

        def sent_home(send, group):
            remote(
                acc.at[0, group, mine], owned.at[1, group],
                home_send.at[send], home_recv.at[0], {"row": far_inner},
            ).wait_send()

        @pl.when(home)
        def _():
            for send in range(2, 2 + 3 * thirds):
                sent_home(send, 0)
            for kind in range(3):
                send_relay(kind).wait_send()

        @pl.when(jnp.logical_not(home))
        def _():
            sent_home(0, every)
            sent_home(1, every)

        arrived_far = pl.ds(near, far)
        arrived_near = pl.ds(0, near)
        for at, source in (
            (0, land.at[0, arrived_far]),
            (1, land.at[0, arrived_far]),
            (2, land.at[0, arrived_near]),
            (3, land.at[1, arrived_far]),
            (4, land.at[2, arrived_far]),
            (5, land.at[3, arrived_far]),
            (6, land.at[1, arrived_near]),
        ):
            remote(
                source, source, sent_sem.at[at], whole_sem.at[0, 0], {"row": far_inner}
            ).wait_send()

    def owned_whole(kind):
        arrived(owned.at[kind, every], kind_sem(kind, 0))

    def owned_thirds(kind):
        for third in range(thirds):
            arrived(owned.at[kind, third], kind_sem(kind, third))

    @pl.when(edge & home)
    def _():
        owned_thirds(1)

    @pl.when(jnp.logical_not(edge) & home)
    def _():
        owned_whole(0)

    @pl.when(edge & jnp.logical_not(home))
    def _():
        owned_whole(0)
        owned_thirds(1)
        owned_thirds(2)

    @pl.when(jnp.logical_not(edge) & jnp.logical_not(home))
    def _():
        owned_whole(0)
        owned_whole(1)
        owned_whole(2)

    for block, value in ((col, owned[0] + owned[2]), (1 - col, owned[1])):
        ladder = value.reshape(out.shape[1:])
        out[block] = ladder
        step_out[block] = ladder / below[block]


def line_exchange(amplitudes, integrals, occ_energy, vir_energy):
    pair_rows = amplitudes.shape[0]
    depth, width = integrals.shape
    chunks = -(-depth // CHUNK)
    near = 3 * chunks // 8
    layers = lax.axis_size("layer")
    slab = width // layers
    thirds = slab // PIECE
    padded = -(-pair_rows // 128) * 128
    group = width // thirds
    vmem = functools.partial(pltpu.VMEM, dtype=jnp.float32)
    smem = functools.partial(pltpu.SMEM, dtype=jnp.float32)
    dma = pltpu.SemaphoreType.DMA
    flops = 2 * 3 * 5 * pair_rows * depth * width
    block = jax.ShapeDtypeStruct((2, slab, padded), jnp.float32)
    results = pl.pallas_call(
        functools.partial(line_kernel, near),
        out_shape=(block, block),
        in_specs=[pl.BlockSpec(memory_space=pl.ANY)] * 4,
        out_specs=[pl.BlockSpec(memory_space=pltpu.VMEM)] * 2,
        scratch_shapes=[
            vmem((chunks, padded, CHUNK)),
            vmem((near, padded, CHUNK)),
            vmem((4, chunks, width, CHUNK)),
            vmem((7, thirds, group, padded)),
            vmem((7, thirds, group // 2, padded)),
            vmem((7, thirds, PIECE, padded)),
            vmem((7, thirds, PIECE, padded)),
            vmem((3, thirds, PIECE, padded)),
            vmem((3, thirds, PIECE, padded)),
            vmem((STAGES + 1, CHUNK, width)),
            vmem((2, slab, padded)),
            vmem((pair_rows, depth - (chunks - 1) * CHUNK)),
            smem(occ_energy.shape),
            smem(vir_energy.shape),
            dma((4,)),
            dma((STAGES + 1,)),
            dma((4, chunks)),
            dma((2, near * thirds)),
            dma((near,)),
            dma((7,)),
            dma((2 + 2 * thirds, 3)),
            dma((2 + 2 * thirds, 3)),
            dma((5 + 3 * thirds,)),
            dma((3 * thirds,)),
            dma((3,)),
        ],
        compiler_params=pltpu.CompilerParams(
            collective_id=0, has_side_effects=True, vmem_limit_bytes=67043328
        ),
        cost_estimate=pl.CostEstimate(
            flops=flops, bytes_accessed=4 * depth * (pair_rows + width), transcendentals=0
        ),
    )(amplitudes, integrals, occ_energy, vir_energy)

    def placed(value):
        return value[:, :, :pair_rows].transpose(0, 2, 1).reshape(2 * pair_rows, slab)

    return tuple(placed(value) for value in results)


def gathered(amplitudes, integrals):
    partial_rows = jnp.dot(
        amplitudes,
        lax.all_gather(integrals, "row", axis=1, tiled=True),
        precision=lax.Precision.HIGHEST,
        preferred_element_type=jnp.float32,
    )
    partial_sum = lax.all_to_all(partial_rows, "row", split_axis=1, concat_axis=0, tiled=True)
    return lax.psum_scatter(
        owner_blocks(partial_sum), ("col", "layer"), scatter_dimension=0, tiled=True
    )


def fits_line(amplitudes, integrals):
    pair_rows = amplitudes.shape[0]
    depth, width = integrals.shape
    chunks = -(-depth // CHUNK)
    near = 3 * chunks // 8
    split_evenly = width % (4 * PIECE) == 0 and pair_rows % 8 == 0 and near % 3 == 0
    words = chunks * (4 * width + pair_rows) + near * pair_rows
    return split_evenly and near >= 9 and words * CHUNK * 4 < 56 * 2**20


def shards(amplitudes, integrals, occ_energy, vir_energy):
    in_line = lax.axis_size("row") == 4 and lax.axis_size("col") == 2
    in_line = in_line and lax.axis_size("layer") == 4
    if in_line and fits_line(amplitudes, integrals):
        return line_exchange(amplitudes, integrals, occ_energy, vir_energy)
    ladder = gathered(amplitudes, integrals)
    pair_rows = ladder.shape[0]
    slab_cols = ladder.shape[1]
    occupied = occ_energy.shape[0]
    virtuals = vir_energy.shape[0]
    first_np, second_np = np.triu_indices(occupied, 1)
    ij_start = lax.axis_index("col") * pair_rows
    ab_start = (
        lax.axis_index("row") * lax.axis_size("layer") + lax.axis_index("layer")
    ) * slab_cols
    first_index = lax.dynamic_slice_in_dim(
        jnp.asarray(first_np, dtype=jnp.int32), ij_start, pair_rows
    )
    second_index = lax.dynamic_slice_in_dim(
        jnp.asarray(second_np, dtype=jnp.int32), ij_start, pair_rows
    )
    pair_sum = lookup(first_index, occ_energy) + lookup(second_index, occ_energy)
    ab_index = ab_start + jnp.arange(slab_cols, dtype=jnp.int32)
    vir_sum = lookup(ab_index // virtuals, vir_energy) + lookup(ab_index % virtuals, vir_energy)
    denominator = pair_sum[:, None] - vir_sum[None, :]
    return (ladder, ladder / denominator)


def solution(mesh):
    in_specs = (P("row", ("layer", "col")), P(("layer", "col"), "row"), P(), P())
    out_specs = (P("col", ("row", "layer")), P("col", ("row", "layer")))
    return jax.shard_map(shards, mesh=mesh, in_specs=in_specs, out_specs=out_specs, check_vma=False)
```

```python
import functools

import jax
import jax.numpy as jnp
import numpy as np
from jax import lax
from jax.experimental import pallas as pl
from jax.experimental.pallas import tpu as pltpu
from jax.sharding import PartitionSpec as P

MESH = pl.DeviceIdType.MESH
CHUNK = 384
PIECE = 16
LAG = 4


def lookup(indices, values_table):
    positions = jnp.arange(values_table.shape[0], dtype=jnp.int32)
    picked = jnp.where(indices[:, None] == positions[None, :], values_table[None, :], 0.0)
    return jnp.sum(picked, axis=1)


def owner_blocks(partial_sum):
    col_count = lax.axis_size("col")
    layer_count = lax.axis_size("layer")
    pair_rows = partial_sum.shape[0] // col_count
    slab_cols = partial_sum.shape[1] // layer_count
    blocks = partial_sum.reshape(col_count, pair_rows, layer_count, slab_cols)
    return blocks.transpose(0, 2, 1, 3).reshape(col_count * layer_count * pair_rows, slab_cols)


def split(value):
    high = value.astype(jnp.bfloat16)
    return high, (value - high.astype(jnp.float32)).astype(jnp.bfloat16)


def product(columns, rows):
    dims = (((1,), (1,)), ((), ()))

    def dot(left, right):
        return lax.dot_general(left, right, dims, preferred_element_type=jnp.float32)

    column_high, column_low = columns
    row_high, row_low = rows
    return (
        dot(column_low, row_high) + dot(column_high, row_low) + dot(column_high, row_high)
    )


def denominators(pair_rows, occ, vir, below):
    row = lax.axis_index("row")
    col = lax.axis_index("col")
    layer = lax.axis_index("layer")
    blocks, slab, lanes = below.shape
    occupied = occ.shape[0]
    virtuals = vir.shape[0]
    shape = (8, lanes)
    block = lax.broadcasted_iota(jnp.int32, shape, 0)
    pair = (blocks * col + block) * pair_rows + lax.broadcasted_iota(jnp.int32, shape, 1)

    def begin(k):
        return k * (2 * occupied - k - 1) // 2

    def pick_first(k, carry):
        energy, second = carry
        inside = (pair >= begin(k)) & (pair < begin(k + 1))
        return (
            energy + jnp.where(inside, occ[k], 0.0),
            jnp.where(inside, pair - begin(k) + k + 1, second),
        )

    zeros = jnp.zeros(shape, jnp.float32)
    first_energy, second = lax.fori_loop(
        0, occupied, pick_first, (zeros, jnp.zeros(shape, jnp.int32))
    )

    def pick_second(k, energy):
        return energy + jnp.where(second == k, occ[k], 0.0)

    pair_sum = first_energy + lax.fori_loop(0, occupied, pick_second, zeros)
    start = (row * lax.axis_size("layer") + layer) * slab

    def fill(i, carry):
        index = start + i
        vir_sum = jnp.full(shape, vir[index // virtuals]) + vir[index % virtuals]
        value = pair_sum - vir_sum
        for at in range(blocks):
            below[at, pl.ds(i, 1)] = value[at : at + 1]
        return carry

    lax.fori_loop(0, slab, fill, 0)


def line_kernel(
    near,
    t_hbm,
    v_hbm,
    occ_hbm,
    vir_hbm,
    out,
    step_out,
    rows,
    lent,
    land,
    acc,
    from_core,
    from_x,
    from_y,
    owned,
    relay,
    below,
    row_tail,
    column_tail,
    occ,
    vir,
    load_sem,
    whole_sem,
    third_sem,
    lent_sem,
    sent_sem,
    hop_send,
    hop_recv,
    home_send,
    home_recv,
    relay_recv,
):
    pair_rows, depth = t_hbm.shape
    chunks = land.shape[1]
    far = chunks - near
    slab = acc.shape[3]
    thirds = slab // PIECE
    row = lax.axis_index("row")
    col = lax.axis_index("col")
    layer = lax.axis_index("layer")
    core = layer % 2
    x_side = layer // 2
    half = row // 2
    edge = (row == 0) | (row == 3)
    home = col == half
    edge_row = 3 * half
    inner_row = 1 + half
    far_inner = 2 - half
    far_edge = 3 - 3 * half
    core_mate = {"layer": x_side * 2 + (1 - core)}
    x_mate = {"layer": (1 - x_side) * 2 + core}
    y_mate = {"col": 1 - col}

    def remote(source, target, send_sem, recv_sem, device):
        return pltpu.make_async_remote_copy(
            src_ref=source,
            dst_ref=target,
            send_sem=send_sem,
            recv_sem=recv_sem,
            device_id=device,
            device_id_type=MESH,
        )

    def arrived(target, sem):
        pltpu.make_async_copy(target, target, sem).wait()

    def third_rows(third):
        return pl.ds(pl.multiple_of(third * PIECE, PIECE), PIECE)

    def depth_at(c):
        return pl.ds(pl.multiple_of(c * CHUNK, CHUNK), CHUNK)

    last_start = (chunks - 1) * CHUNK
    last_depth = depth - last_start
    rows_real = pl.ds(0, pair_rows)
    spare = pl.ds(pair_rows, rows.shape[1] - pair_rows)

    tails = (
        pltpu.make_async_copy(
            v_hbm.at[:, :, :, pl.ds(last_start, last_depth)], column_tail, load_sem.at[0]
        ),
        pltpu.make_async_copy(
            t_hbm.at[:, pl.ds(last_start, last_depth)], row_tail, load_sem.at[1]
        ),
        pltpu.make_async_copy(occ_hbm, occ, load_sem.at[2]),
        pltpu.make_async_copy(vir_hbm, vir, load_sem.at[3]),
    )
    barrier = pltpu.get_barrier_semaphore()
    owned[...] = jnp.zeros_like(owned)
    for step in range(1, 4):
        pl.semaphore_signal(
            barrier, inc=1, device_id={"row": (row + step) % 4}, device_id_type=MESH
        )
    for mate in (core_mate, x_mate, y_mate):
        pl.semaphore_signal(barrier, inc=1, device_id=mate, device_id_type=MESH)
    for copy in tails:
        copy.start()
    land[0, chunks - 1] = jnp.zeros_like(land[0, chunks - 1])
    tails[0].wait()
    land[0, chunks - 1, :, :, :, pl.ds(0, last_depth)] = column_tail[...]

    def send_far(source, c):
        @pl.when(edge)
        def _():
            remote(
                source, land.at[1, c], sent_sem.at[0], whole_sem.at[1, c],
                {"row": inner_row},
            ).start()

        @pl.when(jnp.logical_not(edge))
        def _():
            remote(
                source, land.at[2, c], sent_sem.at[0], whole_sem.at[2, c],
                {"row": far_inner},
            ).start()
            remote(
                source, land.at[1, c], sent_sem.at[1], whole_sem.at[1, c],
                {"row": edge_row},
            ).start()

    pl.semaphore_wait(barrier, 6)

    def far_loop(c, carry):
        send_far(v_hbm.at[:, :, :, depth_at(c)], c)
        return carry

    lax.fori_loop(near, chunks - 1, far_loop, 0)
    send_far(land.at[0, chunks - 1], chunks - 1)

    @pl.when(edge)
    def _():
        def send_lent(c, carry):
            remote(
                t_hbm.at[:, depth_at(c)], lent.at[c, rows_real], sent_sem.at[1],
                lent_sem.at[c], {"row": inner_row},
            ).start()
            return carry

        def send_piece(n, carry):
            third, c = n // near, n % near
            remote(
                v_hbm.at[:, :, third_rows(third), depth_at(c)],
                land.at[1, c, :, :, third_rows(third)],
                sent_sem.at[2], third_sem.at[0, n], {"row": inner_row},
            ).start()
            return carry

        lax.fori_loop(0, near, send_lent, 0)
        lax.fori_loop(0, near * thirds, send_piece, 0)

    @pl.when(jnp.logical_not(edge))
    def _():
        def send_near(c, carry):
            remote(
                v_hbm.at[:, :, :, depth_at(c)], land.at[2, c], sent_sem.at[2],
                whole_sem.at[2, c], {"row": far_inner},
            ).start()
            return carry

        lax.fori_loop(0, near, send_near, 0)

    def load_chunk(c, carry):
        pltpu.make_async_copy(
            t_hbm.at[:, depth_at(c)], rows.at[c, rows_real], load_sem.at[4]
        ).start()
        pltpu.make_async_copy(
            v_hbm.at[:, :, :, depth_at(c)], land.at[0, c], load_sem.at[5]
        ).start()
        return carry

    lax.fori_loop(0, chunks - 1, load_chunk, 0)
    acc[...] = jnp.zeros_like(acc)
    rows[chunks - 1] = jnp.zeros_like(rows[chunks - 1])

    def clear_rows(c, carry):
        rows[c, spare] = jnp.zeros_like(rows[c, spare])
        return carry

    def clear_lent(c, carry):
        lent[c, spare] = jnp.zeros_like(lent[c, spare])
        return carry

    lax.fori_loop(0, chunks - 1, clear_rows, 0)
    lax.fori_loop(0, near, clear_lent, 0)
    for copy in tails[1:]:
        copy.wait()
    rows[chunks - 1, rows_real, pl.ds(0, last_depth)] = row_tail[...]
    denominators(pair_rows, occ, vir, below)
    loaded = pl.ds(0, chunks - 1)
    arrived(rows.at[loaded, rows_real], load_sem.at[4])
    arrived(land.at[0, loaded], load_sem.at[5])

    def add_whole(block, c, pairs):
        other = split(block[c])
        for slot, part in pairs:
            columns = land[part, c].reshape(-1, CHUNK)
            acc[slot] += product(split(columns), other).reshape(acc.shape[1:])

    def add_third(block, c, third, pairs):
        other = split(block[c])
        for slot, part in pairs:
            at = third_rows(third)
            columns = land[part, c, :, :, at].reshape(-1, CHUNK)
            sums = product(split(columns), other)
            acc[slot, :, :, at] += sums.reshape(2, 2, PIECE, -1)

    class Unit:
        def __init__(self, index, slots, group, here, there):
            self.index, self.slots, self.group = index, slots, group
            self.here, self.there = here, there
            self.slot_here, self.slot_there = here is not None, there is not None
            if self.slot_here and self.slot_there:
                self.kept = jnp.where(home, here, there)
                self.given = jnp.where(home, there, here)
                self.gives = self.takes = True
            else:
                self.kept = self.given = slots
                self.takes = home if self.slot_here else jnp.logical_not(home)
                self.gives = jnp.logical_not(self.takes)

        def core_copy(self):
            return remote(
                acc.at[self.slots, :, 1 - core, self.group],
                from_core.at[self.slots, :, self.group],
                hop_send.at[self.index, 0], hop_recv.at[self.index, 0], core_mate,
            )

        def x_copy(self):
            return remote(
                acc.at[self.slots, 1 - x_side, core, self.group],
                from_x.at[self.slots, self.group],
                hop_send.at[self.index, 1], hop_recv.at[self.index, 1], x_mate,
            )

        def y_copy(self):
            return remote(
                acc.at[self.given, x_side, core, self.group],
                from_y.at[self.given, self.group],
                hop_send.at[self.index, 2], hop_recv.at[self.index, 2], y_mate,
            )

        def start(self):
            self.core_copy().start()

        def second(self):
            self.core_copy().wait()
            at = (self.slots, slice(None), core, self.group)
            acc[at] += from_core[self.slots, :, self.group]
            self.x_copy().start()

        def third(self):
            self.x_copy().wait()
            acc[self.slots, x_side, core, self.group] += from_x[self.slots, self.group]
            when(self.gives, lambda: self.y_copy().start())

        def last(self, targets_here, targets_there=()):
            when(self.gives, lambda: self.y_copy().wait_send())

            def take():
                self.y_copy().wait_recv()
                at = (self.kept, x_side, core, self.group)
                acc[at] += from_y[self.kept, self.group]

            when(self.takes, take)

            def deliver(targets):
                for slot, target, device, send, recv in targets:
                    source = acc.at[slot, x_side, core, self.group]
                    if device is None:
                        target[self.group] = source[...]
                    else:
                        remote(
                            source, target.at[self.group], home_send.at[send], recv,
                            {"row": device},
                        ).start()

            if targets_here:
                pl.when(home)(lambda: deliver(targets_here))
            if targets_there:
                pl.when(jnp.logical_not(home))(lambda: deliver(targets_there))

        def run(self, targets_here, targets_there=()):
            self.start()
            self.second()
            self.third()
            self.last(targets_here, targets_there)

    def when(condition, action):
        if condition is True:
            action()
        else:
            pl.when(condition)(action)

    every = pl.ds(0, slab)

    def kind_sem(kind, group):
        return home_recv.at[kind * thirds + group]

    @pl.when(edge)
    def _():
        def own(c, carry):
            add_whole(rows, c, ((0, 0),))
            return carry

        def other(part, i, carry):
            c = near + i
            arrived(land.at[part, c], whole_sem.at[part, c])
            add_whole(rows, c, ((part, part),))
            return carry

        lax.fori_loop(0, chunks, own, 0)
        lax.fori_loop(0, far, functools.partial(other, 1), 0)
        Unit(0, pl.ds(0, 2), every, 0, None).run(
            (
                (0, owned.at[0], None, 0, None),
                (1, owned.at[0], inner_row, 0, kind_sem(0, 0)),
            )
        )
        lax.fori_loop(0, far, functools.partial(other, 2), 0)
        Unit(1, pl.ds(2, 1), every, None, 2).run(
            (), ((2, relay.at[0], far_inner, 1, relay_recv.at[0]),)
        )
        lax.fori_loop(0, far, functools.partial(other, 3), 0)
        Unit(2, pl.ds(3, 1), every, 3, None).run(
            ((3, owned.at[0], far_edge, 2, kind_sem(0, 0)),)
        )

        def sent_home(send, group):
            remote(
                acc.at[0, x_side, core, group], owned.at[0, group],
                home_send.at[send], home_recv.at[0], {"row": inner_row},
            ).wait_send()

        @pl.when(home)
        def _():
            sent_home(0, every)
            sent_home(2, every)

        @pl.when(jnp.logical_not(home))
        def _():
            sent_home(1, every)

        arrived_far = pl.ds(near, far)
        for at, source in (
            (0, land.at[0, arrived_far]), (2, land.at[0, pl.ds(0, near)]),
        ):
            remote(
                source, source, sent_sem.at[at], whole_sem.at[0, 0], {"row": inner_row}
            ).wait_send()
        remote(
            rows.at[pl.ds(0, near), rows_real], rows.at[pl.ds(0, near), rows_real],
            sent_sem.at[1], whole_sem.at[0, 0], {"row": inner_row},
        ).wait_send()

    @pl.when(jnp.logical_not(edge))
    def _():
        def first_far(i, carry):
            c = near + i
            arrived(land.at[1, c], whole_sem.at[1, c])
            remote(
                land.at[1, c], land.at[3, c], sent_sem.at[3], whole_sem.at[3, c],
                {"row": far_inner},
            ).start()
            arrived(land.at[2, c], whole_sem.at[2, c])
            remote(
                land.at[2, c], land.at[2, c], sent_sem.at[4], whole_sem.at[2, c],
                {"row": edge_row},
            ).start()
            add_whole(rows, c, ((0, 0), (4, 1), (1, 2)))
            return carry

        def first_near(c, carry):
            arrived(land.at[2, c], whole_sem.at[2, c])
            add_whole(rows, c, ((0, 0), (1, 2)))
            return carry

        def lent_chunk(c, carry):
            arrived(lent.at[c, rows_real], lent_sem.at[c])
            add_whole(lent, c, ((2, 0), (3, 2)))
            return carry

        def second_far(i, carry):
            c = near + i
            arrived(land.at[3, c], whole_sem.at[3, c])
            remote(
                land.at[3, c], land.at[3, c], sent_sem.at[5], whole_sem.at[3, c],
                {"row": edge_row},
            ).start()
            add_whole(rows, c, ((5, 3),))
            return carry

        lax.fori_loop(0, far, first_far, 0)
        early = near // 3

        def early_block(m, carry):
            lax.fori_loop(3 * m, 3 * m + 3, first_near, 0)
            return lent_chunk(m, carry)

        lax.fori_loop(0, early, early_block, 0)
        Unit(0, pl.ds(0, 2), every, 0, 1).run(
            ((0, owned.at[1], None, 0, None),),
            ((1, relay.at[1], far_inner, 0, relay_recv.at[1]),),
        )
        late = near - early
        per = far // (late - 1)

        def late_block(m, carry):
            lax.fori_loop(per * m, per * m + per, second_far, 0)
            return lent_chunk(early + m, carry)

        lax.fori_loop(0, late - 1, late_block, 0)
        lax.fori_loop(per * (late - 1), far, second_far, 0)
        lent_chunk(near - 1, 0)

        lent_unit = Unit(1, pl.ds(2, 2), every, 2, 3)
        lent_targets = (
            ((2, owned.at[2], None, 0, None),),
            ((3, relay.at[2], far_inner, 1, relay_recv.at[2]),),
        )

        def edge_unit(third):
            return Unit(2 + third, pl.ds(4, 1), third_rows(third), 4, None)

        def edge_targets(third):
            return ((4, owned.at[1], edge_row, 2 + third, kind_sem(1, third)),)

        def last_unit(third):
            return Unit(2 + thirds + third, pl.ds(5, 2), third_rows(third), 5, None)

        def last_targets(third):
            return (
                (5, owned.at[1], far_edge, 2 + thirds + third, kind_sem(1, third)),
                (6, owned.at[2], far_edge, 2 + 2 * thirds + third, kind_sem(2, third)),
            )

        pieces = near * thirds

        def pass_on(n):
            third, c = n // near, n % near
            at = third_rows(third)
            arrived(land.at[1, c, :, :, at], third_sem.at[0, n])
            remote(
                land.at[1, c, :, :, at], land.at[3, c, :, :, at],
                sent_sem.at[6], third_sem.at[1, n], {"row": far_inner},
            ).start()
            add_third(rows, c, third, ((4, 1),))

        def near_step(n, carry):
            third, c = n // near, n % near

            @pl.when(n + LAG < pieces)
            def _():
                pass_on(n + LAG)

            arrived(land.at[3, c, :, :, third_rows(third)], third_sem.at[1, n])
            add_third(rows, c, third, ((5, 3),))
            add_third(lent, c, third, ((6, 3),))

            first = third == 0
            later = jnp.logical_not(first)
            before = third - 1
            pl.when(first & (c == 1))(lent_unit.start)
            pl.when(first & (c == 3))(lent_unit.second)
            pl.when(first & (c == 5))(lent_unit.third)
            pl.when(first & (c == 7))(lambda: lent_unit.last(*lent_targets))
            pl.when(later & (c == 1))(lambda: last_unit(before).start())
            pl.when(later & (c == 3))(lambda: last_unit(before).second())
            pl.when(later & (c == 5))(lambda: last_unit(before).third())
            pl.when(later & (c == 7))(
                lambda: last_unit(before).last(last_targets(before))
            )
            pl.when(c == near - LAG)(lambda: edge_unit(third).start())
            pl.when(c == near - LAG + 2)(lambda: edge_unit(third).second())
            pl.when(later & (c == 0))(lambda: edge_unit(before).third())
            pl.when(later & (c == 2))(
                lambda: edge_unit(before).last(edge_targets(before))
            )
            return carry

        def send_relay(kind):
            return remote(
                relay.at[kind], owned.at[kind], home_send.at[2 + 3 * thirds + kind],
                kind_sem(kind, 0), y_mate,
            )

        def relay_on(kind):
            @pl.when(home)
            def _():
                arrived(relay.at[kind], relay_recv.at[kind])
                send_relay(kind).start()

        for n in range(LAG):
            pass_on(n)
        lax.fori_loop(0, pieces, near_step, 0)
        final = thirds - 1
        last_unit(final).start()
        edge_unit(final).third()
        relay_on(1)
        last_unit(final).second()
        edge_unit(final).last(edge_targets(final))
        relay_on(2)
        last_unit(final).third()
        last_unit(final).last(last_targets(final))
        relay_on(0)

        def sent_home(send, group):
            remote(
                acc.at[0, x_side, core, group], owned.at[1, group],
                home_send.at[send], home_recv.at[0], {"row": far_inner},
            ).wait_send()

        @pl.when(home)
        def _():
            for send in range(2, 2 + 3 * thirds):
                sent_home(send, third_rows(0))
            for kind in range(3):
                send_relay(kind).wait_send()

        @pl.when(jnp.logical_not(home))
        def _():
            sent_home(0, every)
            sent_home(1, every)

        arrived_far = pl.ds(near, far)
        arrived_near = pl.ds(0, near)
        for at, source in (
            (0, land.at[0, arrived_far]),
            (1, land.at[0, arrived_far]),
            (2, land.at[0, arrived_near]),
            (3, land.at[1, arrived_far]),
            (4, land.at[2, arrived_far]),
            (5, land.at[3, arrived_far]),
            (6, land.at[1, arrived_near]),
        ):
            remote(
                source, source, sent_sem.at[at], whole_sem.at[0, 0], {"row": far_inner}
            ).wait_send()

    def owned_whole(kind):
        arrived(owned.at[kind, every], kind_sem(kind, 0))

    def owned_thirds(kind):
        for third in range(thirds):
            arrived(owned.at[kind, third_rows(third)], kind_sem(kind, third))

    @pl.when(edge & home)
    def _():
        owned_thirds(1)

    @pl.when(jnp.logical_not(edge) & home)
    def _():
        owned_whole(0)

    @pl.when(edge & jnp.logical_not(home))
    def _():
        owned_whole(0)
        owned_thirds(1)
        owned_thirds(2)

    @pl.when(jnp.logical_not(edge) & jnp.logical_not(home))
    def _():
        owned_whole(0)
        owned_whole(1)
        owned_whole(2)

    edge_sum = owned[0] + owned[2]
    inner_sum = owned[1]
    real = slice(0, pair_rows)
    for block, own_col in ((0, col == 0), (1, col == 1)):
        ladder = jnp.where(own_col, edge_sum, inner_sum)
        step = ladder / below[block]
        lanes = pl.ds(block * pair_rows, pair_rows)
        out[:, lanes] = ladder[:, real]
        step_out[:, lanes] = step[:, real]


def line_exchange(amplitudes, integrals, occ_energy, vir_energy):
    pair_rows = amplitudes.shape[0]
    depth, width = integrals.shape
    chunks = -(-depth // CHUNK)
    near = 3 * chunks // 8
    layers = lax.axis_size("layer")
    slab = width // layers
    thirds = slab // PIECE
    padded = -(-pair_rows // 128) * 128
    last_depth = depth - (chunks - 1) * CHUNK
    vmem = functools.partial(pltpu.VMEM, dtype=jnp.float32)
    smem = functools.partial(pltpu.SMEM, dtype=jnp.float32)
    dma = pltpu.SemaphoreType.DMA
    flops = 2 * 3 * 5 * pair_rows * depth * width
    block = jax.ShapeDtypeStruct((slab, 2 * pair_rows), jnp.float32)
    columns = integrals.T.reshape(layers // 2, 2, slab, depth)
    results = pl.pallas_call(
        functools.partial(line_kernel, near),
        out_shape=(block, block),
        in_specs=[pl.BlockSpec(memory_space=pl.ANY)] * 4,
        out_specs=[pl.BlockSpec(memory_space=pltpu.VMEM)] * 2,
        scratch_shapes=[
            vmem((chunks, padded, CHUNK)),
            vmem((near, padded, CHUNK)),
            vmem((4, chunks, 2, 2, slab, CHUNK)),
            vmem((7, 2, 2, slab, padded)),
            vmem((7, 2, slab, padded)),
            vmem((7, slab, padded)),
            vmem((7, slab, padded)),
            vmem((3, slab, padded)),
            vmem((3, slab, padded)),
            vmem((2, slab, padded)),
            vmem((pair_rows, last_depth)),
            vmem((2, 2, slab, last_depth)),
            smem(occ_energy.shape),
            smem(vir_energy.shape),
            dma((6,)),
            dma((4, chunks)),
            dma((2, near * thirds)),
            dma((near,)),
            dma((7,)),
            dma((2 + 2 * thirds, 3)),
            dma((2 + 2 * thirds, 3)),
            dma((5 + 3 * thirds,)),
            dma((3 * thirds,)),
            dma((3,)),
        ],
        compiler_params=pltpu.CompilerParams(
            collective_id=0, has_side_effects=True, vmem_limit_bytes=67043328
        ),
        cost_estimate=pl.CostEstimate(
            flops=flops, bytes_accessed=4 * depth * (pair_rows + width), transcendentals=0
        ),
    )(amplitudes, columns, occ_energy, vir_energy)
    return tuple(value.T for value in results)


def gathered(amplitudes, integrals):
    partial_rows = jnp.dot(
        amplitudes,
        lax.all_gather(integrals, "row", axis=1, tiled=True),
        precision=lax.Precision.HIGHEST,
        preferred_element_type=jnp.float32,
    )
    partial_sum = lax.all_to_all(partial_rows, "row", split_axis=1, concat_axis=0, tiled=True)
    return lax.psum_scatter(
        owner_blocks(partial_sum), ("col", "layer"), scatter_dimension=0, tiled=True
    )


def fits_line(amplitudes, integrals):
    pair_rows = amplitudes.shape[0]
    depth, width = integrals.shape
    chunks = -(-depth // CHUNK)
    near = 3 * chunks // 8
    split_evenly = width % (4 * PIECE) == 0 and pair_rows % 8 == 0 and near % 3 == 0
    words = chunks * (4 * width + pair_rows) + near * pair_rows
    return split_evenly and near >= 9 and words * CHUNK * 4 < 56 * 2**20


def shards(amplitudes, integrals, occ_energy, vir_energy):
    in_line = lax.axis_size("row") == 4 and lax.axis_size("col") == 2
    in_line = in_line and lax.axis_size("layer") == 4
    if in_line and fits_line(amplitudes, integrals):
        return line_exchange(amplitudes, integrals, occ_energy, vir_energy)
    ladder = gathered(amplitudes, integrals)
    pair_rows = ladder.shape[0]
    slab_cols = ladder.shape[1]
    occupied = occ_energy.shape[0]
    virtuals = vir_energy.shape[0]
    first_np, second_np = np.triu_indices(occupied, 1)
    ij_start = lax.axis_index("col") * pair_rows
    ab_start = (
        lax.axis_index("row") * lax.axis_size("layer") + lax.axis_index("layer")
    ) * slab_cols
    first_index = lax.dynamic_slice_in_dim(
        jnp.asarray(first_np, dtype=jnp.int32), ij_start, pair_rows
    )
    second_index = lax.dynamic_slice_in_dim(
        jnp.asarray(second_np, dtype=jnp.int32), ij_start, pair_rows
    )
    pair_sum = lookup(first_index, occ_energy) + lookup(second_index, occ_energy)
    ab_index = ab_start + jnp.arange(slab_cols, dtype=jnp.int32)
    vir_sum = lookup(ab_index // virtuals, vir_energy) + lookup(ab_index % virtuals, vir_energy)
    denominator = pair_sum[:, None] - vir_sum[None, :]
    return (ladder, ladder / denominator)


def solution(mesh):
    in_specs = (P("row", ("layer", "col")), P(("layer", "col"), "row"), P(), P())
    out_specs = (P("col", ("row", "layer")), P("col", ("row", "layer")))
    return jax.shard_map(shards, mesh=mesh, in_specs=in_specs, out_specs=out_specs, check_vma=False)
```

```python
import functools

import jax
import jax.numpy as jnp
import numpy as np
from jax import lax
from jax.experimental import pallas as pl
from jax.experimental.pallas import tpu as pltpu
from jax.sharding import PartitionSpec as P

MESH = pl.DeviceIdType.MESH
CHUNK = 256
LAG = 8


def lookup(indices, values_table):
    positions = jnp.arange(values_table.shape[0], dtype=jnp.int32)
    picked = jnp.where(indices[:, None] == positions[None, :], values_table[None, :], 0.0)
    return jnp.sum(picked, axis=1)


def owner_blocks(partial_sum):
    col_count = lax.axis_size("col")
    layer_count = lax.axis_size("layer")
    pair_rows = partial_sum.shape[0] // col_count
    slab_cols = partial_sum.shape[1] // layer_count
    blocks = partial_sum.reshape(col_count, pair_rows, layer_count, slab_cols)
    return blocks.transpose(0, 2, 1, 3).reshape(col_count * layer_count * pair_rows, slab_cols)


def near_chunks(chunks):
    return -(-5 * chunks // 14)


def groups_of(slab):
    return ((0, slab - 24), (slab - 24, 16), (slab - 8, 8))


def split(value):
    high = value.astype(jnp.bfloat16)
    return high, (value - high.astype(jnp.float32)).astype(jnp.bfloat16)


def product(columns, rows):
    dims = (((1,), (1,)), ((), ()))

    def dot(left, right):
        return lax.dot_general(left, right, dims, preferred_element_type=jnp.float32)

    column_high, column_low = columns
    row_high, row_low = rows
    return (
        dot(column_low, row_high) + dot(column_high, row_low) + dot(column_high, row_high)
    )


def denominators(pair_rows, occ, vir, below):
    row = lax.axis_index("row")
    col = lax.axis_index("col")
    layer = lax.axis_index("layer")
    blocks, slab, lanes = below.shape
    occupied = occ.shape[0]
    virtuals = vir.shape[0]
    shape = (8, lanes)
    block = lax.broadcasted_iota(jnp.int32, shape, 0)
    pair = (blocks * col + block) * pair_rows + lax.broadcasted_iota(jnp.int32, shape, 1)

    def begin(k):
        return k * (2 * occupied - k - 1) // 2

    def pick_first(k, carry):
        energy, second = carry
        inside = (pair >= begin(k)) & (pair < begin(k + 1))
        return (
            energy + jnp.where(inside, occ[k], 0.0),
            jnp.where(inside, pair - begin(k) + k + 1, second),
        )

    zeros = jnp.zeros(shape, jnp.float32)
    first_energy, second = lax.fori_loop(
        0, occupied, pick_first, (zeros, jnp.zeros(shape, jnp.int32))
    )

    def pick_second(k, energy):
        return energy + jnp.where(second == k, occ[k], 0.0)

    pair_sum = first_energy + lax.fori_loop(0, occupied, pick_second, zeros)
    start = (row * lax.axis_size("layer") + layer) * slab

    def fill(i, carry):
        index = start + i
        vir_sum = jnp.full(shape, vir[index // virtuals]) + vir[index % virtuals]
        value = pair_sum - vir_sum
        for at in range(blocks):
            below[at, pl.ds(i, 1)] = value[at : at + 1]
        return carry

    lax.fori_loop(0, slab, fill, 0)


def line_kernel(
    near,
    t_hbm,
    v_hbm,
    occ_hbm,
    vir_hbm,
    out,
    rows,
    lent,
    land,
    acc,
    from_core,
    from_x,
    from_y,
    owned,
    relay,
    below,
    row_tail,
    column_tail,
    occ,
    vir,
    load_sem,
    whole_sem,
    third_sem,
    lent_sem,
    sent_sem,
    hop_send,
    hop_recv,
    home_send,
    home_recv,
    relay_recv,
    go_sem,
):
    pair_rows, depth = t_hbm.shape
    chunks = land.shape[1]
    far = chunks - near
    slab = acc.shape[3]
    groups = groups_of(slab)
    thirds = len(groups)
    row = lax.axis_index("row")
    col = lax.axis_index("col")
    layer = lax.axis_index("layer")
    core = layer % 2
    x_side = layer // 2
    half = row // 2
    edge = (row == 0) | (row == 3)
    home = col == half
    edge_row = 3 * half
    inner_row = 1 + half
    far_inner = 2 - half
    far_edge = 3 - 3 * half
    core_mate = {"layer": x_side * 2 + (1 - core)}
    x_mate = {"layer": (1 - x_side) * 2 + core}
    y_mate = {"col": 1 - col}

    def remote(source, target, send_sem, recv_sem, device):
        return pltpu.make_async_remote_copy(
            src_ref=source,
            dst_ref=target,
            send_sem=send_sem,
            recv_sem=recv_sem,
            device_id=device,
            device_id_type=MESH,
        )

    def arrived(target, sem):
        pltpu.make_async_copy(target, target, sem).wait()

    def third_rows(third):
        return pl.ds(*groups[third])

    def depth_at(c):
        return pl.ds(pl.multiple_of(c * CHUNK, CHUNK), CHUNK)

    last_start = (chunks - 1) * CHUNK
    last_depth = depth - last_start
    rows_real = pl.ds(0, pair_rows)
    spare = pl.ds(pair_rows, rows.shape[1] - pair_rows)

    tails = (
        pltpu.make_async_copy(
            v_hbm.at[:, :, :, pl.ds(last_start, last_depth)], column_tail, load_sem.at[0]
        ),
        pltpu.make_async_copy(
            t_hbm.at[:, pl.ds(last_start, last_depth)], row_tail, load_sem.at[1]
        ),
        pltpu.make_async_copy(occ_hbm, occ, load_sem.at[2]),
        pltpu.make_async_copy(vir_hbm, vir, load_sem.at[3]),
    )
    barrier = pltpu.get_barrier_semaphore()
    owned[...] = jnp.zeros_like(owned)
    for step in range(1, 4):
        pl.semaphore_signal(
            barrier, inc=1, device_id={"row": (row + step) % 4}, device_id_type=MESH
        )
    for mate in (core_mate, x_mate, y_mate):
        pl.semaphore_signal(barrier, inc=1, device_id=mate, device_id_type=MESH)
    for copy in tails:
        copy.start()
    land[0, chunks - 1] = jnp.zeros_like(land[0, chunks - 1])
    tails[0].wait()
    land[0, chunks - 1, :, :, :, pl.ds(0, last_depth)] = column_tail[...]

    def send_far(source, c):
        @pl.when(edge)
        def _():
            remote(
                source, land.at[1, c], sent_sem.at[0], whole_sem.at[c - near],
                {"row": inner_row},
            ).start()

        @pl.when(jnp.logical_not(edge))
        def _():
            remote(
                source, land.at[2, c], sent_sem.at[0], whole_sem.at[far + c],
                {"row": far_inner},
            ).start()
            remote(
                source, land.at[1, c], sent_sem.at[1], whole_sem.at[c - near],
                {"row": edge_row},
            ).start()

    pl.semaphore_wait(barrier, 6)

    def far_loop(c, carry):
        send_far(v_hbm.at[:, :, :, depth_at(c)], c)
        return carry

    lax.fori_loop(near, chunks - 1, far_loop, 0)
    send_far(land.at[0, chunks - 1], chunks - 1)

    @pl.when(edge)
    def _():
        def send_lent(c, carry):
            remote(
                t_hbm.at[:, depth_at(c)], lent.at[c, rows_real], sent_sem.at[1],
                lent_sem.at[c], {"row": inner_row},
            ).start()
            return carry

        def send_piece(third, c, carry):
            remote(
                v_hbm.at[:, :, third_rows(third), depth_at(c)],
                land.at[1, c, :, :, third_rows(third)],
                sent_sem.at[2], third_sem.at[0, third * near + c], {"row": inner_row},
            ).start()
            return carry

        lax.fori_loop(0, near, send_lent, 0)
        for third in range(thirds):
            lax.fori_loop(0, near, functools.partial(send_piece, third), 0)

    @pl.when(jnp.logical_not(edge))
    def _():
        def send_near(c, carry):
            remote(
                v_hbm.at[:, :, :, depth_at(c)], land.at[2, c], sent_sem.at[2],
                whole_sem.at[far + c], {"row": far_inner},
            ).start()
            return carry

        lax.fori_loop(0, near, send_near, 0)

    def load_chunk(c, carry):
        pltpu.make_async_copy(
            t_hbm.at[:, depth_at(c)], rows.at[c, rows_real], load_sem.at[4]
        ).start()
        pltpu.make_async_copy(
            v_hbm.at[:, :, :, depth_at(c)], land.at[0, c], load_sem.at[5]
        ).start()
        return carry

    lax.fori_loop(0, chunks - 1, load_chunk, 0)
    acc[...] = jnp.zeros_like(acc)
    rows[chunks - 1] = jnp.zeros_like(rows[chunks - 1])

    def clear_rows(c, carry):
        rows[c, spare] = jnp.zeros_like(rows[c, spare])
        return carry

    def clear_lent(c, carry):
        lent[c, spare] = jnp.zeros_like(lent[c, spare])
        return carry

    lax.fori_loop(0, chunks - 1, clear_rows, 0)
    lax.fori_loop(0, near, clear_lent, 0)
    for copy in tails[1:]:
        copy.wait()
    rows[chunks - 1, rows_real, pl.ds(0, last_depth)] = row_tail[...]
    denominators(pair_rows, occ, vir, below)
    loaded = pl.ds(0, chunks - 1)
    arrived(rows.at[loaded, rows_real], load_sem.at[4])
    arrived(land.at[0, loaded], load_sem.at[5])

    def add_whole(block, c, pairs):
        other = split(block[c])
        for slot, part in pairs:
            columns = land[part, c].reshape(-1, CHUNK)
            acc[slot] += product(split(columns), other).reshape(acc.shape[1:])

    def add_third(block, c, third, pairs):
        other = split(block[c])
        for slot, part in pairs:
            at = third_rows(third)
            columns = land[part, c, :, :, at].reshape(-1, CHUNK)
            sums = product(split(columns), other)
            acc[slot, :, :, at] += sums.reshape(2, 2, at.size, -1)

    class Unit:
        def __init__(self, index, slots, group, here, there):
            self.index, self.slots, self.group = index, slots, group
            self.here, self.there = here, there
            self.slot_here, self.slot_there = here is not None, there is not None
            if self.slot_here and self.slot_there:
                self.kept = jnp.where(home, here, there)
                self.given = jnp.where(home, there, here)
                self.gives = self.takes = True
            else:
                self.kept = self.given = slots
                self.takes = home if self.slot_here else jnp.logical_not(home)
                self.gives = jnp.logical_not(self.takes)

        def core_copy(self):
            return remote(
                acc.at[self.slots, :, 1 - core, self.group],
                from_core.at[self.slots, :, self.group],
                hop_send.at[self.index, 0], hop_recv.at[self.index, 0], core_mate,
            )

        def x_copy(self):
            return remote(
                acc.at[self.slots, 1 - x_side, core, self.group],
                from_x.at[self.slots, self.group],
                hop_send.at[self.index, 1], hop_recv.at[self.index, 1], x_mate,
            )

        def y_copy(self):
            return remote(
                acc.at[self.given, x_side, core, self.group],
                from_y.at[self.given, self.group],
                hop_send.at[self.index, 2], hop_recv.at[self.index, 2], y_mate,
            )

        def start(self):
            self.core_copy().start()

        def second(self):
            self.core_copy().wait()
            at = (self.slots, slice(None), core, self.group)
            acc[at] += from_core[self.slots, :, self.group]
            self.x_copy().start()

        def third(self):
            self.x_copy().wait()
            acc[self.slots, x_side, core, self.group] += from_x[self.slots, self.group]
            when(self.gives, lambda: self.y_copy().start())

        def last(self, targets_here, targets_there=()):
            when(self.gives, lambda: self.y_copy().wait_send())

            def take():
                self.y_copy().wait_recv()
                at = (self.kept, x_side, core, self.group)
                acc[at] += from_y[self.kept, self.group]

            when(self.takes, take)

            self.deliver(targets_here, targets_there)

        def deliver(self, targets_here, targets_there=()):
            def go(targets):
                for slot, target, device, send, recv in targets:
                    source = acc.at[slot, x_side, core, self.group]
                    if device is None:
                        target[self.group] = source[...]
                    else:
                        remote(
                            source, target.at[self.group], home_send.at[send], recv,
                            {"row": device},
                        ).start()

            if targets_here:
                pl.when(home)(lambda: go(targets_here))
            if targets_there:
                pl.when(jnp.logical_not(home))(lambda: go(targets_there))

        def run(self, targets_here, targets_there=()):
            self.start()
            self.second()
            self.third()
            self.last(targets_here, targets_there)

    def when(condition, action):
        if condition is True:
            action()
        else:
            pl.when(condition)(action)

    every = pl.ds(0, slab)

    def owned_whole(kind):
        arrived(owned.at[kind, every], kind_sem(kind, 0))

    def owned_third(kind, third):
        arrived(owned.at[kind, third_rows(third)], kind_sem(kind, third))

    def put(block, at, value):
        lanes = pl.ds(block * pair_rows, pair_rows)
        real = slice(0, pair_rows)
        out[0, at, lanes] = value[:, real]
        out[1, at, lanes] = (value / below[block, at])[:, real]

    def put_edge(at):
        for block in range(2):
            pl.when(col == block)(lambda: put(block, at, owned[0, at] + owned[2, at]))

    def put_inner(at):
        for block in range(2):
            pl.when(col != block)(lambda: put(block, at, owned[1, at]))

    def kind_sem(kind, group):
        return home_recv.at[kind * thirds + group]

    @pl.when(edge)
    def _():
        def own(c, carry):
            add_whole(rows, c, ((0, 0),))
            return carry

        def other(part, i, carry):
            c = near + i
            first = (0, far + near, far + chunks)[part - 1]
            arrived(land.at[part, c], whole_sem.at[first + i])
            add_whole(rows, c, ((part, part),))
            return carry

        lax.fori_loop(0, chunks, own, 0)
        lax.fori_loop(0, far, functools.partial(other, 1), 0)
        Unit(0, pl.ds(0, 2), every, 0, None).run(
            (
                (0, owned.at[0], None, 0, None),
                (1, owned.at[0], inner_row, 0, kind_sem(0, 0)),
            )
        )
        lax.fori_loop(0, far, functools.partial(other, 2), 0)
        second_unit = Unit(1, pl.ds(2, 1), every, None, 2)
        second_unit.run(())
        lax.fori_loop(0, far, functools.partial(other, 3), 0)
        Unit(2, pl.ds(3, 1), every, 3, None).run(())
        pl.semaphore_wait(go_sem, 1)
        second_unit.deliver(
            ((3, owned.at[0], far_edge, 2, kind_sem(0, 0)),),
            ((2, relay.at[0], far_inner, 1, relay_recv.at[0]),),
        )

        def sent_home(send, group):
            remote(
                acc.at[0, x_side, core, group], owned.at[0, group],
                home_send.at[send], home_recv.at[0], {"row": inner_row},
            ).wait_send()

        @pl.when(home)
        def _():
            sent_home(0, every)
            sent_home(2, every)

        @pl.when(jnp.logical_not(home))
        def _():
            sent_home(1, every)

        arrived_far = pl.ds(near, far)
        for at, source in (
            (0, land.at[0, arrived_far]), (2, land.at[0, pl.ds(0, near)]),
        ):
            remote(
                source, source, sent_sem.at[at], whole_sem.at[0], {"row": inner_row}
            ).wait_send()
        remote(
            rows.at[pl.ds(0, near), rows_real], rows.at[pl.ds(0, near), rows_real],
            sent_sem.at[1], whole_sem.at[0], {"row": inner_row},
        ).wait_send()

    @pl.when(jnp.logical_not(edge))
    def _():
        def first_far(i, carry):
            c = near + i
            arrived(land.at[1, c], whole_sem.at[c - near])
            remote(
                land.at[1, c], land.at[3, c], sent_sem.at[3], whole_sem.at[far + chunks + c - near],
                {"row": far_inner},
            ).start()
            arrived(land.at[2, c], whole_sem.at[far + c])
            remote(
                land.at[2, c], land.at[2, c], sent_sem.at[4], whole_sem.at[far + c],
                {"row": edge_row},
            ).start()
            add_whole(rows, c, ((0, 0), (4, 1), (1, 2)))
            return carry

        def first_near(c, carry):
            arrived(land.at[2, c], whole_sem.at[far + c])
            add_whole(rows, c, ((0, 0), (1, 2)))
            return carry

        def lent_chunk(c, carry):
            arrived(lent.at[c, rows_real], lent_sem.at[c])
            add_whole(lent, c, ((2, 0), (3, 2)))
            return carry

        def second_far(c, carry):
            arrived(land.at[3, c], whole_sem.at[far + chunks + c - near])
            remote(
                land.at[3, c], land.at[3, c], sent_sem.at[5], whole_sem.at[far + chunks + c - near],
                {"row": edge_row},
            ).start()
            add_whole(rows, c, ((5, 3),))
            return carry

        lax.fori_loop(0, far, first_far, 0)

        def lent_due(step):
            due = (8 * step - 1) // 21
            return jnp.where(step < 1, 0, jnp.minimum(due, near))

        def with_lent(body, step, carry):
            body(step, carry)
            count = lent_due(step)

            @pl.when(count > lent_due(step - 1))
            def _():
                lent_chunk(count - 1, 0)

            return carry

        lax.fori_loop(0, near, functools.partial(with_lent, first_near), 0)
        own_unit = Unit(0, pl.ds(0, 2), every, 0, 1)
        own_unit.run(((0, owned.at[1], None, 0, None),))
        lax.fori_loop(near, chunks, functools.partial(with_lent, second_far), 0)
        left = near - (8 * (chunks - 1) - 1) // 21
        for j in range(max(left, 0)):
            lent_chunk(near - left + j, 0)

        lent_unit = Unit(1, pl.ds(2, 2), every, 2, 3)
        own_targets = ((1, relay.at[1], far_inner, 0, relay_recv.at[1]),)
        lent_targets = ((3, relay.at[2], far_inner, 1, relay_recv.at[2]),)

        def edge_unit(third):
            return Unit(2 + third, pl.ds(4, 1), third_rows(third), 4, None)

        def edge_targets(third):
            return ((4, owned.at[1], edge_row, 2 + third, kind_sem(1, third)),)

        def last_unit(third):
            return Unit(2 + thirds + third, pl.ds(5, 2), third_rows(third), 5, None)

        def last_targets(third):
            return (
                (5, owned.at[1], far_edge, 2 + thirds + third, kind_sem(1, third)),
                (6, owned.at[2], far_edge, 2 + 2 * thirds + third, kind_sem(2, third)),
            )

        def pass_on(third, c):
            n = third * near + c
            at = third_rows(third)
            arrived(land.at[1, c, :, :, at], third_sem.at[0, n])
            remote(
                land.at[1, c, :, :, at], land.at[3, c, :, :, at],
                sent_sem.at[6], third_sem.at[1, n], {"row": far_inner},
            ).start()
            add_third(rows, c, third, ((4, 1),))

        def near_step(third, c, carry):
            ahead = c + LAG
            pl.when(ahead < near)(lambda: pass_on(third, ahead))
            if third + 1 < thirds:
                pl.when(ahead >= near)(lambda: pass_on(third + 1, ahead - near))
            at = third_rows(third)
            arrived(land.at[3, c, :, :, at], third_sem.at[1, third * near + c])
            add_third(rows, c, third, ((5, 3),))
            add_third(lent, c, third, ((6, 3),))

            def stage(step, action):
                pl.when(c == step)(action)

            if third == 0:
                stage(0, lent_unit.start)
                stage(2, lent_unit.second)
                stage(6, lent_unit.third)
                stage(10, lambda: lent_unit.last(((2, owned.at[2], None, 0, None),)))
            else:
                before = third - 1
                late = before + 2 == thirds
                stage(0, last_unit(before).start)
                stage(2, last_unit(before).second)
                stage(7, last_unit(before).third)
                if not late:
                    stage(near - 1, lambda: last_unit(before).last(()))
                stage(1, edge_unit(before).third)
                stage(5, lambda: edge_unit(before).last(edge_targets(before)))
            stage(near - LAG, edge_unit(third).start)
            stage(near - LAG + 2, edge_unit(third).second)
            if third + 1 == thirds:
                stage(near - LAG, cross)
            return carry

        def cross():
            pl.semaphore_signal(
                go_sem, inc=1, device_id={"row": edge_row}, device_id_type=MESH
            )
            own_unit.deliver((), own_targets)
            lent_unit.deliver((), lent_targets)
            for third in range(thirds - 2):
                last_unit(third).deliver(last_targets(third))

        def send_relay(kind):
            return remote(
                relay.at[kind], owned.at[kind], home_send.at[2 + 3 * thirds + kind],
                kind_sem(kind, 0), y_mate,
            )

        def relay_on(kind):
            @pl.when(home)
            def _():
                arrived(relay.at[kind], relay_recv.at[kind])
                send_relay(kind).start()

        for c in range(LAG):
            pass_on(0, c)
        for third in range(thirds):
            lax.fori_loop(0, near, functools.partial(near_step, third), 0)
        final = thirds - 1
        last_unit(final).start()
        edge_unit(final).third()
        last_unit(final - 1).last(last_targets(final - 1))
        last_unit(final).second()

        @pl.when(home)
        def _():
            owned_whole(0)
            put_edge(every)
            put_inner(every)

        relay_on(1)
        edge_unit(final).last(edge_targets(final))
        last_unit(final).third()
        relay_on(2)
        relay_on(0)
        last_unit(final).last(last_targets(final))

        def sent_home(send, group):
            remote(
                acc.at[0, x_side, core, group], owned.at[1, group],
                home_send.at[send], home_recv.at[0], {"row": far_inner},
            ).wait_send()

        @pl.when(home)
        def _():
            for at in range(3):
                for third in range(thirds):
                    sent_home(2 + at * thirds + third, third_rows(third))
            for kind in range(3):
                send_relay(kind).wait_send()

        @pl.when(jnp.logical_not(home))
        def _():
            sent_home(0, every)
            sent_home(1, every)

        arrived_far = pl.ds(near, far)
        arrived_near = pl.ds(0, near)
        for at, source in (
            (0, land.at[0, arrived_far]),
            (1, land.at[0, arrived_far]),
            (2, land.at[0, arrived_near]),
            (3, land.at[1, arrived_far]),
            (4, land.at[2, arrived_far]),
            (5, land.at[3, arrived_far]),
            (6, land.at[1, arrived_near]),
        ):
            remote(
                source, source, sent_sem.at[at], whole_sem.at[0], {"row": far_inner}
            ).wait_send()

    @pl.when(edge & home)
    def _():
        put_edge(every)
        for third in range(thirds):
            owned_third(1, third)
            put_inner(third_rows(third))

    @pl.when(edge & jnp.logical_not(home))
    def _():
        owned_whole(0)
        for third in range(thirds):
            owned_third(1, third)
            put_inner(third_rows(third))
            owned_third(2, third)
            put_edge(third_rows(third))

    @pl.when(jnp.logical_not(edge) & jnp.logical_not(home))
    def _():
        owned_whole(1)
        put_inner(every)
        owned_whole(2)
        owned_whole(0)
        put_edge(every)


def line_exchange(amplitudes, integrals, occ_energy, vir_energy):
    pair_rows = amplitudes.shape[0]
    depth, width = integrals.shape
    chunks = -(-depth // CHUNK)
    near = near_chunks(chunks)
    layers = lax.axis_size("layer")
    slab = width // layers
    groups = groups_of(slab)
    thirds = len(groups)
    padded = -(-pair_rows // 128) * 128
    last_depth = depth - (chunks - 1) * CHUNK
    vmem = functools.partial(pltpu.VMEM, dtype=jnp.float32)
    smem = functools.partial(pltpu.SMEM, dtype=jnp.float32)
    dma = pltpu.SemaphoreType.DMA
    flops = 2 * 3 * 5 * pair_rows * depth * width
    columns = integrals.T.reshape(layers // 2, 2, slab, depth)
    result = pl.pallas_call(
        functools.partial(line_kernel, near),
        out_shape=jax.ShapeDtypeStruct((2, slab, 2 * pair_rows), jnp.float32),
        in_specs=[pl.BlockSpec(memory_space=pl.ANY)] * 4,
        out_specs=pl.BlockSpec(memory_space=pltpu.VMEM),
        scratch_shapes=[
            vmem((chunks, padded, CHUNK)),
            vmem((near, padded, CHUNK)),
            vmem((4, chunks, 2, 2, slab, CHUNK)),
            vmem((7, 2, 2, slab, padded)),
            vmem((7, 2, slab, padded)),
            vmem((7, slab, padded)),
            vmem((7, slab, padded)),
            vmem((3, slab, padded)),
            vmem((3, slab, padded)),
            vmem((2, slab, padded)),
            vmem((pair_rows, last_depth)),
            vmem((2, 2, slab, last_depth)),
            smem(occ_energy.shape),
            smem(vir_energy.shape),
            dma((6,)),
            dma((3 * chunks - 2 * near,)),
            dma((2, near * thirds)),
            dma((near,)),
            dma((7,)),
            dma((2 + 2 * thirds, 3)),
            dma((2 + 2 * thirds, 3)),
            dma((5 + 3 * thirds,)),
            dma((3 * thirds,)),
            dma((3,)),
            pltpu.SemaphoreType.REGULAR,
        ],
        compiler_params=pltpu.CompilerParams(
            collective_id=0, has_side_effects=True, vmem_limit_bytes=67043328
        ),
        cost_estimate=pl.CostEstimate(
            flops=flops, bytes_accessed=4 * depth * (pair_rows + width), transcendentals=0
        ),
    )(amplitudes, columns, occ_energy, vir_energy)
    return result[0].T, result[1].T


def gathered(amplitudes, integrals):
    partial_rows = jnp.dot(
        amplitudes,
        lax.all_gather(integrals, "row", axis=1, tiled=True),
        precision=lax.Precision.HIGHEST,
        preferred_element_type=jnp.float32,
    )
    partial_sum = lax.all_to_all(partial_rows, "row", split_axis=1, concat_axis=0, tiled=True)
    return lax.psum_scatter(
        owner_blocks(partial_sum), ("col", "layer"), scatter_dimension=0, tiled=True
    )


def fits_line(amplitudes, integrals):
    pair_rows = amplitudes.shape[0]
    depth, width = integrals.shape
    chunks = -(-depth // CHUNK)
    near = near_chunks(chunks)
    even = width % 32 == 0 and width >= 128 and pair_rows % 8 == 0
    words = chunks * (4 * width + pair_rows) + near * pair_rows
    return even and near >= 13 and words * CHUNK * 4 < 56 * 2**20


def shards(amplitudes, integrals, occ_energy, vir_energy):
    in_line = lax.axis_size("row") == 4 and lax.axis_size("col") == 2
    in_line = in_line and lax.axis_size("layer") == 4
    if in_line and fits_line(amplitudes, integrals):
        return line_exchange(amplitudes, integrals, occ_energy, vir_energy)
    ladder = gathered(amplitudes, integrals)
    pair_rows = ladder.shape[0]
    slab_cols = ladder.shape[1]
    occupied = occ_energy.shape[0]
    virtuals = vir_energy.shape[0]
    first_np, second_np = np.triu_indices(occupied, 1)
    ij_start = lax.axis_index("col") * pair_rows
    ab_start = (
        lax.axis_index("row") * lax.axis_size("layer") + lax.axis_index("layer")
    ) * slab_cols
    first_index = lax.dynamic_slice_in_dim(
        jnp.asarray(first_np, dtype=jnp.int32), ij_start, pair_rows
    )
    second_index = lax.dynamic_slice_in_dim(
        jnp.asarray(second_np, dtype=jnp.int32), ij_start, pair_rows
    )
    pair_sum = lookup(first_index, occ_energy) + lookup(second_index, occ_energy)
    ab_index = ab_start + jnp.arange(slab_cols, dtype=jnp.int32)
    vir_sum = lookup(ab_index // virtuals, vir_energy) + lookup(ab_index % virtuals, vir_energy)
    denominator = pair_sum[:, None] - vir_sum[None, :]
    return (ladder, ladder / denominator)


def solution(mesh):
    in_specs = (P("row", ("layer", "col")), P(("layer", "col"), "row"), P(), P())
    out_specs = (P("col", ("row", "layer")), P("col", ("row", "layer")))
    return jax.shard_map(shards, mesh=mesh, in_specs=in_specs, out_specs=out_specs, check_vma=False)
```

```python
import functools

import jax
import jax.numpy as jnp
import numpy as np
from jax import lax
from jax.experimental import pallas as pl
from jax.experimental.pallas import tpu as pltpu
from jax.sharding import PartitionSpec as P

MESH = pl.DeviceIdType.MESH
CHUNK = 256
LAG = 8


def lookup(indices, values_table):
    positions = jnp.arange(values_table.shape[0], dtype=jnp.int32)
    picked = jnp.where(indices[:, None] == positions[None, :], values_table[None, :], 0.0)
    return jnp.sum(picked, axis=1)


def owner_blocks(partial_sum):
    col_count = lax.axis_size("col")
    layer_count = lax.axis_size("layer")
    pair_rows = partial_sum.shape[0] // col_count
    slab_cols = partial_sum.shape[1] // layer_count
    blocks = partial_sum.reshape(col_count, pair_rows, layer_count, slab_cols)
    return blocks.transpose(0, 2, 1, 3).reshape(col_count * layer_count * pair_rows, slab_cols)


def near_chunks(chunks):
    return -(-5 * chunks // 14)


def groups_of(slab):
    return ((0, slab - 24), (slab - 24, 16), (slab - 8, 8))


def split(value):
    high = value.astype(jnp.bfloat16)
    return high, (value - high.astype(jnp.float32)).astype(jnp.bfloat16)


def product(columns, rows):
    dims = (((1,), (1,)), ((), ()))

    def dot(left, right):
        return lax.dot_general(left, right, dims, preferred_element_type=jnp.float32)

    column_high, column_low = columns
    row_high, row_low = rows
    return (
        dot(column_low, row_high) + dot(column_high, row_low) + dot(column_high, row_high)
    )


def denominators(pair_rows, occ, vir, below):
    row = lax.axis_index("row")
    col = lax.axis_index("col")
    layer = lax.axis_index("layer")
    blocks, slab, lanes = below.shape
    occupied = occ.shape[0]
    virtuals = vir.shape[0]
    shape = (8, lanes)
    block = lax.broadcasted_iota(jnp.int32, shape, 0)
    pair = (blocks * col + block) * pair_rows + lax.broadcasted_iota(jnp.int32, shape, 1)

    def begin(k):
        return k * (2 * occupied - k - 1) // 2

    def pick_first(k, carry):
        energy, second = carry
        inside = (pair >= begin(k)) & (pair < begin(k + 1))
        return (
            energy + jnp.where(inside, occ[k], 0.0),
            jnp.where(inside, pair - begin(k) + k + 1, second),
        )

    zeros = jnp.zeros(shape, jnp.float32)
    first_energy, second = lax.fori_loop(
        0, occupied, pick_first, (zeros, jnp.zeros(shape, jnp.int32))
    )

    def pick_second(k, energy):
        return energy + jnp.where(second == k, occ[k], 0.0)

    pair_sum = first_energy + lax.fori_loop(0, occupied, pick_second, zeros)
    start = (row * lax.axis_size("layer") + layer) * slab

    def fill(i, carry):
        index = start + i
        vir_sum = jnp.full(shape, vir[index // virtuals]) + vir[index % virtuals]
        value = pair_sum - vir_sum
        for at in range(blocks):
            below[at, pl.ds(i, 1)] = value[at : at + 1]
        return carry

    lax.fori_loop(0, slab, fill, 0)


def line_kernel(
    near,
    t_hbm,
    v_hbm,
    occ_hbm,
    vir_hbm,
    out,
    rows,
    lent,
    land,
    acc,
    from_core,
    from_x,
    from_y,
    from_cross,
    owned,
    relay,
    below,
    row_tail,
    column_tail,
    occ,
    vir,
    load_sem,
    whole_sem,
    third_sem,
    lent_sem,
    sent_sem,
    hop_send,
    hop_recv,
    home_send,
    home_recv,
    relay_recv,
    go_sem,
):
    pair_rows, depth = t_hbm.shape
    chunks = land.shape[1]
    far = chunks - near
    slab = acc.shape[3]
    groups = groups_of(slab)
    thirds = len(groups)
    row = lax.axis_index("row")
    col = lax.axis_index("col")
    layer = lax.axis_index("layer")
    core = layer % 2
    x_side = layer // 2
    half = row // 2
    edge = (row == 0) | (row == 3)
    home = col == half
    edge_row = 3 * half
    inner_row = 1 + half
    far_inner = 2 - half
    far_edge = 3 - 3 * half
    core_mate = {"layer": x_side * 2 + (1 - core)}
    x_mate = {"layer": (1 - x_side) * 2 + core}
    y_mate = {"col": 1 - col}
    cross_mate = {"col": 1 - col, "layer": (1 - x_side) * 2 + core}

    def remote(source, target, send_sem, recv_sem, device):
        return pltpu.make_async_remote_copy(
            src_ref=source,
            dst_ref=target,
            send_sem=send_sem,
            recv_sem=recv_sem,
            device_id=device,
            device_id_type=MESH,
        )

    def arrived(target, sem):
        pltpu.make_async_copy(target, target, sem).wait()

    def third_rows(third):
        return pl.ds(*groups[third])

    def depth_at(c):
        return pl.ds(pl.multiple_of(c * CHUNK, CHUNK), CHUNK)

    last_start = (chunks - 1) * CHUNK
    last_depth = depth - last_start
    rows_real = pl.ds(0, pair_rows)
    spare = pl.ds(pair_rows, rows.shape[1] - pair_rows)

    tails = (
        pltpu.make_async_copy(
            v_hbm.at[:, :, :, pl.ds(last_start, last_depth)], column_tail, load_sem.at[0]
        ),
        pltpu.make_async_copy(
            t_hbm.at[:, pl.ds(last_start, last_depth)], row_tail, load_sem.at[1]
        ),
        pltpu.make_async_copy(occ_hbm, occ, load_sem.at[2]),
        pltpu.make_async_copy(vir_hbm, vir, load_sem.at[3]),
    )
    barrier = pltpu.get_barrier_semaphore()
    owned[...] = jnp.zeros_like(owned)
    for step in range(1, 4):
        pl.semaphore_signal(
            barrier, inc=1, device_id={"row": (row + step) % 4}, device_id_type=MESH
        )
    for mate in (core_mate, x_mate, y_mate, cross_mate):
        pl.semaphore_signal(barrier, inc=1, device_id=mate, device_id_type=MESH)
    for copy in tails:
        copy.start()
    land[0, chunks - 1] = jnp.zeros_like(land[0, chunks - 1])
    tails[0].wait()
    land[0, chunks - 1, :, :, :, pl.ds(0, last_depth)] = column_tail[...]

    def send_far(source, c):
        @pl.when(edge)
        def _():
            remote(
                source, land.at[1, c], sent_sem.at[0], whole_sem.at[c - near],
                {"row": inner_row},
            ).start()

        @pl.when(jnp.logical_not(edge))
        def _():
            remote(
                source, land.at[2, c], sent_sem.at[0], whole_sem.at[far + c],
                {"row": far_inner},
            ).start()
            remote(
                source, land.at[1, c], sent_sem.at[1], whole_sem.at[c - near],
                {"row": edge_row},
            ).start()

    pl.semaphore_wait(barrier, 7)

    def far_loop(c, carry):
        send_far(v_hbm.at[:, :, :, depth_at(c)], c)
        return carry

    lax.fori_loop(near, chunks - 1, far_loop, 0)
    send_far(land.at[0, chunks - 1], chunks - 1)

    @pl.when(edge)
    def _():
        def send_lent(c, carry):
            remote(
                t_hbm.at[:, depth_at(c)], lent.at[c, rows_real], sent_sem.at[1],
                lent_sem.at[c], {"row": inner_row},
            ).start()
            return carry

        def send_piece(third, c, carry):
            remote(
                v_hbm.at[:, :, third_rows(third), depth_at(c)],
                land.at[1, c, :, :, third_rows(third)],
                sent_sem.at[2], third_sem.at[0, third * near + c], {"row": inner_row},
            ).start()
            return carry

        lax.fori_loop(0, near, send_lent, 0)
        for third in range(thirds):
            lax.fori_loop(0, near, functools.partial(send_piece, third), 0)

    @pl.when(jnp.logical_not(edge))
    def _():
        def send_near(c, carry):
            remote(
                v_hbm.at[:, :, :, depth_at(c)], land.at[2, c], sent_sem.at[2],
                whole_sem.at[far + c], {"row": far_inner},
            ).start()
            return carry

        lax.fori_loop(0, near, send_near, 0)

    def load_chunk(c, carry):
        pltpu.make_async_copy(
            t_hbm.at[:, depth_at(c)], rows.at[c, rows_real], load_sem.at[4]
        ).start()
        pltpu.make_async_copy(
            v_hbm.at[:, :, :, depth_at(c)], land.at[0, c], load_sem.at[5]
        ).start()
        return carry

    lax.fori_loop(0, chunks - 1, load_chunk, 0)
    acc[...] = jnp.zeros_like(acc)
    rows[chunks - 1] = jnp.zeros_like(rows[chunks - 1])

    def clear_rows(c, carry):
        rows[c, spare] = jnp.zeros_like(rows[c, spare])
        return carry

    def clear_lent(c, carry):
        lent[c, spare] = jnp.zeros_like(lent[c, spare])
        return carry

    lax.fori_loop(0, chunks - 1, clear_rows, 0)
    lax.fori_loop(0, near, clear_lent, 0)
    for copy in tails[1:]:
        copy.wait()
    rows[chunks - 1, rows_real, pl.ds(0, last_depth)] = row_tail[...]
    denominators(pair_rows, occ, vir, below)
    loaded = pl.ds(0, chunks - 1)
    arrived(rows.at[loaded, rows_real], load_sem.at[4])
    arrived(land.at[0, loaded], load_sem.at[5])

    def add_whole(block, c, pairs):
        other = split(block[c])
        for slot, part in pairs:
            columns = land[part, c].reshape(-1, CHUNK)
            acc[slot] += product(split(columns), other).reshape(acc.shape[1:])

    def add_third(block, c, third, pairs):
        other = split(block[c])
        for slot, part in pairs:
            at = third_rows(third)
            columns = land[part, c, :, :, at].reshape(-1, CHUNK)
            sums = product(split(columns), other)
            acc[slot, :, :, at] += sums.reshape(2, 2, at.size, -1)

    class Unit:
        def __init__(self, index, slots, group, here, there):
            self.index, self.slots, self.group = index, slots, group
            self.here, self.there = here, there
            self.slot_here, self.slot_there = here is not None, there is not None
            if self.slot_here and self.slot_there:
                self.kept = jnp.where(home, here, there)
                self.given = jnp.where(home, there, here)
                self.gives = self.takes = True
            else:
                self.kept = self.given = slots
                self.takes = home if self.slot_here else jnp.logical_not(home)
                self.gives = jnp.logical_not(self.takes)

        def core_copy(self):
            return remote(
                acc.at[self.slots, :, 1 - core, self.group],
                from_core.at[self.slots, :, self.group],
                hop_send.at[self.index, 0], hop_recv.at[self.index, 0], core_mate,
            )

        def x_copy(self):
            return remote(
                acc.at[self.slots, 1 - x_side, core, self.group],
                from_x.at[self.slots, self.group],
                hop_send.at[self.index, 1], hop_recv.at[self.index, 1], x_mate,
            )

        def y_copy(self):
            return remote(
                acc.at[self.given, x_side, core, self.group],
                from_y.at[self.given, self.group],
                hop_send.at[self.index, 2], hop_recv.at[self.index, 2], y_mate,
            )

        def start(self):
            self.core_copy().start()

        def second(self):
            self.core_copy().wait()
            at = (self.slots, slice(None), core, self.group)
            acc[at] += from_core[self.slots, :, self.group]
            self.x_copy().start()

        def third(self):
            self.x_copy().wait()
            acc[self.slots, x_side, core, self.group] += from_x[self.slots, self.group]
            when(self.gives, lambda: self.y_copy().start())

        def last(self, targets_here, targets_there=()):
            when(self.gives, lambda: self.y_copy().wait_send())

            def take():
                self.y_copy().wait_recv()
                at = (self.kept, x_side, core, self.group)
                acc[at] += from_y[self.kept, self.group]

            when(self.takes, take)

            self.deliver(targets_here, targets_there)

        def deliver(self, targets_here, targets_there=()):
            def go(targets):
                for slot, target, device, send, recv in targets:
                    source = acc.at[slot, x_side, core, self.group]
                    if device is None:
                        target[self.group] = source[...]
                    else:
                        remote(
                            source, target.at[self.group], home_send.at[send], recv,
                            {"row": device},
                        ).start()

            if targets_here:
                pl.when(home)(lambda: go(targets_here))
            if targets_there:
                pl.when(jnp.logical_not(home))(lambda: go(targets_there))

        def cross_copy(self):
            return remote(
                acc.at[self.slots, 1 - x_side, core, self.group], from_cross,
                hop_send.at[0, 3], hop_recv.at[0, 3], cross_mate,
            )

        def scatter(self):
            self.core_copy().wait()
            at = (self.slots, slice(None), core, self.group)
            acc[at] += from_core[self.slots, :, self.group]
            when(home, lambda: self.x_copy().start())

            @pl.when(jnp.logical_not(home))
            def _():
                self.cross_copy().start()
                self.y_copy().start()

        def gather(self, targets):
            @pl.when(home)
            def _():
                self.x_copy().wait()
                self.y_copy().wait_recv()
                at = (self.slots, x_side, core, self.group)
                near_sum = from_x[self.slots, self.group] + from_y[self.slots, self.group]
                self.cross_copy().wait_recv()
                acc[at] += near_sum + from_cross[...]

            @pl.when(jnp.logical_not(home))
            def _():
                self.y_copy().wait_send()
                self.cross_copy().wait_send()

            self.deliver(targets)

        def run(self, targets_here, targets_there=()):
            self.start()
            self.second()
            self.third()
            self.last(targets_here, targets_there)

    def when(condition, action):
        if condition is True:
            action()
        else:
            pl.when(condition)(action)

    every = pl.ds(0, slab)

    def owned_whole(kind):
        arrived(owned.at[kind, every], kind_sem(kind, 0))

    def owned_third(kind, third):
        arrived(owned.at[kind, third_rows(third)], kind_sem(kind, third))

    def put(block, at, value):
        lanes = pl.ds(block * pair_rows, pair_rows)
        real = slice(0, pair_rows)
        out[0, at, lanes] = value[:, real]
        out[1, at, lanes] = (value / below[block, at])[:, real]

    def put_edge(at):
        for block in range(2):
            pl.when(col == block)(lambda: put(block, at, owned[0, at] + owned[2, at]))

    def put_inner(at):
        for block in range(2):
            pl.when(col != block)(lambda: put(block, at, owned[1, at]))

    def kind_sem(kind, group):
        return home_recv.at[kind * thirds + group]

    @pl.when(edge)
    def _():
        def own(c, carry):
            add_whole(rows, c, ((0, 0),))
            return carry

        def other(part, i, carry):
            c = near + i
            first = (0, far + near, far + chunks)[part - 1]
            arrived(land.at[part, c], whole_sem.at[first + i])
            add_whole(rows, c, ((part, part),))
            return carry

        lax.fori_loop(0, chunks, own, 0)
        lax.fori_loop(0, far, functools.partial(other, 1), 0)
        Unit(0, pl.ds(0, 2), every, 0, None).run(
            (
                (0, owned.at[0], None, 0, None),
                (1, owned.at[0], inner_row, 0, kind_sem(0, 0)),
            )
        )
        lax.fori_loop(0, far, functools.partial(other, 2), 0)
        second_unit = Unit(1, pl.ds(2, 1), every, None, 2)
        second_unit.run(())
        lax.fori_loop(0, far, functools.partial(other, 3), 0)
        Unit(2, pl.ds(3, 1), every, 3, None).run(())
        pl.semaphore_wait(go_sem, 1)
        second_unit.deliver(
            ((3, owned.at[0], far_edge, 2, kind_sem(0, 0)),),
            ((2, relay.at[0], far_inner, 1, relay_recv.at[0]),),
        )

        def sent_home(send, group):
            remote(
                acc.at[0, x_side, core, group], owned.at[0, group],
                home_send.at[send], home_recv.at[0], {"row": inner_row},
            ).wait_send()

        @pl.when(home)
        def _():
            sent_home(0, every)
            sent_home(2, every)

        @pl.when(jnp.logical_not(home))
        def _():
            sent_home(1, every)

        arrived_far = pl.ds(near, far)
        for at, source in (
            (0, land.at[0, arrived_far]), (2, land.at[0, pl.ds(0, near)]),
        ):
            remote(
                source, source, sent_sem.at[at], whole_sem.at[0], {"row": inner_row}
            ).wait_send()
        remote(
            rows.at[pl.ds(0, near), rows_real], rows.at[pl.ds(0, near), rows_real],
            sent_sem.at[1], whole_sem.at[0], {"row": inner_row},
        ).wait_send()

    @pl.when(jnp.logical_not(edge))
    def _():
        def first_far(i, carry):
            c = near + i
            arrived(land.at[1, c], whole_sem.at[c - near])
            remote(
                land.at[1, c], land.at[3, c], sent_sem.at[3], whole_sem.at[far + chunks + c - near],
                {"row": far_inner},
            ).start()
            arrived(land.at[2, c], whole_sem.at[far + c])
            remote(
                land.at[2, c], land.at[2, c], sent_sem.at[4], whole_sem.at[far + c],
                {"row": edge_row},
            ).start()
            add_whole(rows, c, ((0, 0), (4, 1), (1, 2)))
            return carry

        def first_near(c, carry):
            arrived(land.at[2, c], whole_sem.at[far + c])
            add_whole(rows, c, ((0, 0), (1, 2)))
            return carry

        def lent_chunk(c, carry):
            arrived(lent.at[c, rows_real], lent_sem.at[c])
            add_whole(lent, c, ((2, 0), (3, 2)))
            return carry

        def second_far(c, carry):
            arrived(land.at[3, c], whole_sem.at[far + chunks + c - near])
            remote(
                land.at[3, c], land.at[3, c], sent_sem.at[5], whole_sem.at[far + chunks + c - near],
                {"row": edge_row},
            ).start()
            add_whole(rows, c, ((5, 3),))
            return carry

        lax.fori_loop(0, far, first_far, 0)

        def lent_due(step):
            due = (8 * step - 1) // 21
            return jnp.where(step < 1, 0, jnp.minimum(due, near))

        def with_lent(body, step, carry):
            body(step, carry)
            count = lent_due(step)

            @pl.when(count > lent_due(step - 1))
            def _():
                lent_chunk(count - 1, 0)

            return carry

        lax.fori_loop(0, near, functools.partial(with_lent, first_near), 0)
        own_unit = Unit(0, pl.ds(0, 2), every, 0, 1)
        own_unit.run(((0, owned.at[1], None, 0, None),))
        lax.fori_loop(near, chunks, functools.partial(with_lent, second_far), 0)
        left = near - (8 * (chunks - 1) - 1) // 21
        for j in range(max(left, 0)):
            lent_chunk(near - left + j, 0)

        lent_unit = Unit(1, pl.ds(2, 2), every, 2, 3)
        own_targets = ((1, relay.at[1], far_inner, 0, relay_recv.at[1]),)
        lent_targets = ((3, relay.at[2], far_inner, 1, relay_recv.at[2]),)

        def edge_unit(third):
            return Unit(2 + third, pl.ds(4, 1), third_rows(third), 4, None)

        def edge_targets(third):
            return ((4, owned.at[1], edge_row, 2 + third, kind_sem(1, third)),)

        def last_unit(third):
            return Unit(2 + thirds + third, pl.ds(5, 2), third_rows(third), 5, None)

        def last_targets(third):
            return (
                (5, owned.at[1], far_edge, 2 + thirds + third, kind_sem(1, third)),
                (6, owned.at[2], far_edge, 2 + 2 * thirds + third, kind_sem(2, third)),
            )

        def pass_on(third, c):
            n = third * near + c
            at = third_rows(third)
            arrived(land.at[1, c, :, :, at], third_sem.at[0, n])
            remote(
                land.at[1, c, :, :, at], land.at[3, c, :, :, at],
                sent_sem.at[6], third_sem.at[1, n], {"row": far_inner},
            ).start()
            add_third(rows, c, third, ((4, 1),))

        def near_step(third, c, carry):
            ahead = c + LAG
            pl.when(ahead < near)(lambda: pass_on(third, ahead))
            if third + 1 < thirds:
                pl.when(ahead >= near)(lambda: pass_on(third + 1, ahead - near))
            at = third_rows(third)
            arrived(land.at[3, c, :, :, at], third_sem.at[1, third * near + c])
            add_third(rows, c, third, ((5, 3),))
            add_third(lent, c, third, ((6, 3),))

            def stage(step, action):
                pl.when(c == step)(action)

            if third == 0:
                stage(0, lent_unit.start)
                stage(2, lent_unit.second)
                stage(6, lent_unit.third)
                stage(10, lambda: lent_unit.last(((2, owned.at[2], None, 0, None),)))
            else:
                before = third - 1
                late = before + 2 == thirds
                stage(0, last_unit(before).start)
                stage(2, last_unit(before).second)
                stage(7, last_unit(before).third)
                if not late:
                    stage(near - 1, lambda: last_unit(before).last(()))
                stage(1, edge_unit(before).third)
                stage(5, lambda: edge_unit(before).last(edge_targets(before)))
            stage(near - LAG, edge_unit(third).start)
            stage(near - LAG + 2, edge_unit(third).second)
            if third + 1 == thirds:
                stage(near - LAG, cross)
            return carry

        def cross():
            pl.semaphore_signal(
                go_sem, inc=1, device_id={"row": edge_row}, device_id_type=MESH
            )
            own_unit.deliver((), own_targets)
            lent_unit.deliver((), lent_targets)
            for third in range(thirds - 2):
                last_unit(third).deliver(last_targets(third))

        def send_relay(kind):
            return remote(
                relay.at[kind], owned.at[kind], home_send.at[2 + 3 * thirds + kind],
                kind_sem(kind, 0), y_mate,
            )

        def relay_on(kind):
            @pl.when(home)
            def _():
                arrived(relay.at[kind], relay_recv.at[kind])
                send_relay(kind).start()

        for c in range(LAG):
            pass_on(0, c)
        for third in range(thirds):
            lax.fori_loop(0, near, functools.partial(near_step, third), 0)
        final = thirds - 1
        last_unit(final).start()
        edge_unit(final).third()
        last_unit(final - 1).last(last_targets(final - 1))
        last_unit(final).scatter()

        @pl.when(home)
        def _():
            owned_whole(0)
            put_edge(every)
            put_inner(every)

        relay_on(1)
        edge_unit(final).last(edge_targets(final))

        @pl.when(home)
        def _():
            for kind in (2, 0):
                arrived(relay.at[kind], relay_recv.at[kind])
            relay[2] += relay[0]
            send_relay(2).start()

        last_unit(final).gather(last_targets(final))

        def sent_home(send, group):
            remote(
                acc.at[0, x_side, core, group], owned.at[1, group],
                home_send.at[send], home_recv.at[0], {"row": far_inner},
            ).wait_send()

        @pl.when(home)
        def _():
            for at in range(3):
                for third in range(thirds):
                    sent_home(2 + at * thirds + third, third_rows(third))
            for kind in (1, 2):
                send_relay(kind).wait_send()

        @pl.when(jnp.logical_not(home))
        def _():
            sent_home(0, every)
            sent_home(1, every)

        arrived_far = pl.ds(near, far)
        arrived_near = pl.ds(0, near)
        for at, source in (
            (0, land.at[0, arrived_far]),
            (1, land.at[0, arrived_far]),
            (2, land.at[0, arrived_near]),
            (3, land.at[1, arrived_far]),
            (4, land.at[2, arrived_far]),
            (5, land.at[3, arrived_far]),
            (6, land.at[1, arrived_near]),
        ):
            remote(
                source, source, sent_sem.at[at], whole_sem.at[0], {"row": far_inner}
            ).wait_send()

    @pl.when(edge & home)
    def _():
        put_edge(every)
        for third in range(thirds):
            owned_third(1, third)
            put_inner(third_rows(third))

    @pl.when(edge & jnp.logical_not(home))
    def _():
        owned_whole(0)
        for third in range(thirds):
            owned_third(1, third)
            put_inner(third_rows(third))
            owned_third(2, third)
            put_edge(third_rows(third))

    @pl.when(jnp.logical_not(edge) & jnp.logical_not(home))
    def _():
        owned_whole(1)
        put_inner(every)
        owned_whole(2)
        put_edge(every)


def line_exchange(amplitudes, integrals, occ_energy, vir_energy):
    pair_rows = amplitudes.shape[0]
    depth, width = integrals.shape
    chunks = -(-depth // CHUNK)
    near = near_chunks(chunks)
    layers = lax.axis_size("layer")
    slab = width // layers
    groups = groups_of(slab)
    thirds = len(groups)
    padded = -(-pair_rows // 128) * 128
    last_depth = depth - (chunks - 1) * CHUNK
    vmem = functools.partial(pltpu.VMEM, dtype=jnp.float32)
    smem = functools.partial(pltpu.SMEM, dtype=jnp.float32)
    dma = pltpu.SemaphoreType.DMA
    flops = 2 * 3 * 5 * pair_rows * depth * width
    columns = integrals.T.reshape(layers // 2, 2, slab, depth)
    result = pl.pallas_call(
        functools.partial(line_kernel, near),
        out_shape=jax.ShapeDtypeStruct((2, slab, 2 * pair_rows), jnp.float32),
        in_specs=[pl.BlockSpec(memory_space=pl.ANY)] * 4,
        out_specs=pl.BlockSpec(memory_space=pltpu.VMEM),
        scratch_shapes=[
            vmem((chunks, padded, CHUNK)),
            vmem((near, padded, CHUNK)),
            vmem((4, chunks, 2, 2, slab, CHUNK)),
            vmem((7, 2, 2, slab, padded)),
            vmem((7, 2, slab, padded)),
            vmem((7, slab, padded)),
            vmem((7, slab, padded)),
            vmem((2, groups[-1][1], padded)),
            vmem((3, slab, padded)),
            vmem((3, slab, padded)),
            vmem((2, slab, padded)),
            vmem((pair_rows, last_depth)),
            vmem((2, 2, slab, last_depth)),
            smem(occ_energy.shape),
            smem(vir_energy.shape),
            dma((6,)),
            dma((3 * chunks - 2 * near,)),
            dma((2, near * thirds)),
            dma((near,)),
            dma((7,)),
            dma((2 + 2 * thirds, 4)),
            dma((2 + 2 * thirds, 4)),
            dma((5 + 3 * thirds,)),
            dma((3 * thirds,)),
            dma((3,)),
            pltpu.SemaphoreType.REGULAR,
        ],
        compiler_params=pltpu.CompilerParams(
            collective_id=0, has_side_effects=True, vmem_limit_bytes=67043328
        ),
        cost_estimate=pl.CostEstimate(
            flops=flops, bytes_accessed=4 * depth * (pair_rows + width), transcendentals=0
        ),
    )(amplitudes, columns, occ_energy, vir_energy)
    return result[0].T, result[1].T


def gathered(amplitudes, integrals):
    partial_rows = jnp.dot(
        amplitudes,
        lax.all_gather(integrals, "row", axis=1, tiled=True),
        precision=lax.Precision.HIGHEST,
        preferred_element_type=jnp.float32,
    )
    partial_sum = lax.all_to_all(partial_rows, "row", split_axis=1, concat_axis=0, tiled=True)
    return lax.psum_scatter(
        owner_blocks(partial_sum), ("col", "layer"), scatter_dimension=0, tiled=True
    )


def fits_line(amplitudes, integrals):
    pair_rows = amplitudes.shape[0]
    depth, width = integrals.shape
    chunks = -(-depth // CHUNK)
    near = near_chunks(chunks)
    even = width % 32 == 0 and width >= 128 and pair_rows % 8 == 0
    words = chunks * (4 * width + pair_rows) + near * pair_rows
    return even and near >= 13 and words * CHUNK * 4 < 56 * 2**20


def shards(amplitudes, integrals, occ_energy, vir_energy):
    in_line = lax.axis_size("row") == 4 and lax.axis_size("col") == 2
    in_line = in_line and lax.axis_size("layer") == 4
    if in_line and fits_line(amplitudes, integrals):
        return line_exchange(amplitudes, integrals, occ_energy, vir_energy)
    ladder = gathered(amplitudes, integrals)
    pair_rows = ladder.shape[0]
    slab_cols = ladder.shape[1]
    occupied = occ_energy.shape[0]
    virtuals = vir_energy.shape[0]
    first_np, second_np = np.triu_indices(occupied, 1)
    ij_start = lax.axis_index("col") * pair_rows
    ab_start = (
        lax.axis_index("row") * lax.axis_size("layer") + lax.axis_index("layer")
    ) * slab_cols
    first_index = lax.dynamic_slice_in_dim(
        jnp.asarray(first_np, dtype=jnp.int32), ij_start, pair_rows
    )
    second_index = lax.dynamic_slice_in_dim(
        jnp.asarray(second_np, dtype=jnp.int32), ij_start, pair_rows
    )
    pair_sum = lookup(first_index, occ_energy) + lookup(second_index, occ_energy)
    ab_index = ab_start + jnp.arange(slab_cols, dtype=jnp.int32)
    vir_sum = lookup(ab_index // virtuals, vir_energy) + lookup(ab_index % virtuals, vir_energy)
    denominator = pair_sum[:, None] - vir_sum[None, :]
    return (ladder, ladder / denominator)


def solution(mesh):
    in_specs = (P("row", ("layer", "col")), P(("layer", "col"), "row"), P(), P())
    out_specs = (P("col", ("row", "layer")), P("col", ("row", "layer")))
    return jax.shard_map(shards, mesh=mesh, in_specs=in_specs, out_specs=out_specs, check_vma=False)
```

```python
import functools

import jax
import jax.numpy as jnp
import numpy as np
from jax import lax
from jax.experimental import pallas as pl
from jax.experimental.pallas import tpu as pltpu
from jax.sharding import PartitionSpec as P

MESH = pl.DeviceIdType.MESH
CHUNK = 256
LAG = 10


def lookup(indices, values_table):
    positions = jnp.arange(values_table.shape[0], dtype=jnp.int32)
    picked = jnp.where(indices[:, None] == positions[None, :], values_table[None, :], 0.0)
    return jnp.sum(picked, axis=1)


def owner_blocks(partial_sum):
    col_count = lax.axis_size("col")
    layer_count = lax.axis_size("layer")
    pair_rows = partial_sum.shape[0] // col_count
    slab_cols = partial_sum.shape[1] // layer_count
    blocks = partial_sum.reshape(col_count, pair_rows, layer_count, slab_cols)
    return blocks.transpose(0, 2, 1, 3).reshape(col_count * layer_count * pair_rows, slab_cols)


def near_chunks(chunks):
    return -(-5 * chunks // 14)


def groups_of(slab):
    return ((0, slab - 24), (slab - 24, 16), (slab - 8, 8))


def split(value):
    high = value.astype(jnp.bfloat16)
    return high, (value - high.astype(jnp.float32)).astype(jnp.bfloat16)


def product(columns, rows):
    dims = (((1,), (1,)), ((), ()))

    def dot(left, right):
        return lax.dot_general(left, right, dims, preferred_element_type=jnp.float32)

    column_high, column_low = columns
    row_high, row_low = rows
    return (
        dot(column_low, row_high) + dot(column_high, row_low) + dot(column_high, row_high)
    )


def denominators(pair_rows, occ, vir, below):
    row = lax.axis_index("row")
    col = lax.axis_index("col")
    layer = lax.axis_index("layer")
    blocks, slab, lanes = below.shape
    occupied = occ.shape[0]
    virtuals = vir.shape[0]
    shape = (8, lanes)
    block = lax.broadcasted_iota(jnp.int32, shape, 0)
    pair = (blocks * col + block) * pair_rows + lax.broadcasted_iota(jnp.int32, shape, 1)

    def begin(k):
        return k * (2 * occupied - k - 1) // 2

    def pick_first(k, carry):
        energy, second = carry
        inside = (pair >= begin(k)) & (pair < begin(k + 1))
        return (
            energy + jnp.where(inside, occ[k], 0.0),
            jnp.where(inside, pair - begin(k) + k + 1, second),
        )

    zeros = jnp.zeros(shape, jnp.float32)
    first_energy, second = lax.fori_loop(
        0, occupied, pick_first, (zeros, jnp.zeros(shape, jnp.int32))
    )

    def pick_second(k, energy):
        return energy + jnp.where(second == k, occ[k], 0.0)

    pair_sum = first_energy + lax.fori_loop(0, occupied, pick_second, zeros)
    start = (row * lax.axis_size("layer") + layer) * slab

    def fill(i, carry):
        index = start + i
        vir_sum = jnp.full(shape, vir[index // virtuals]) + vir[index % virtuals]
        value = pair_sum - vir_sum
        for at in range(blocks):
            below[at, pl.ds(i, 1)] = value[at : at + 1]
        return carry

    lax.fori_loop(0, slab, fill, 0)


def line_kernel(
    near,
    t_hbm,
    v_hbm,
    occ_hbm,
    vir_hbm,
    out,
    rows,
    lent,
    land,
    acc,
    from_core,
    from_x,
    from_y,
    from_cross,
    owned,
    relay,
    below,
    row_tail,
    column_tail,
    occ,
    vir,
    load_sem,
    whole_sem,
    third_sem,
    lent_sem,
    sent_sem,
    hop_send,
    hop_recv,
    cross_sem,
    home_send,
    home_recv,
    relay_recv,
    go_sem,
):
    pair_rows, depth = t_hbm.shape
    chunks = land.shape[1]
    far = chunks - near
    slab = acc.shape[3]
    groups = groups_of(slab)
    thirds = len(groups)
    row = lax.axis_index("row")
    col = lax.axis_index("col")
    layer = lax.axis_index("layer")
    core = layer % 2
    x_side = layer // 2
    half = row // 2
    edge = (row == 0) | (row == 3)
    home = col == half
    edge_row = 3 * half
    inner_row = 1 + half
    far_inner = 2 - half
    far_edge = 3 - 3 * half
    core_mate = {"layer": x_side * 2 + (1 - core)}
    x_mate = {"layer": (1 - x_side) * 2 + core}
    y_mate = {"col": 1 - col}
    cross_mate = {"col": 1 - col, "layer": (1 - x_side) * 2 + core}

    def remote(source, target, send_sem, recv_sem, device):
        return pltpu.make_async_remote_copy(
            src_ref=source,
            dst_ref=target,
            send_sem=send_sem,
            recv_sem=recv_sem,
            device_id=device,
            device_id_type=MESH,
        )

    def arrived(target, sem):
        pltpu.make_async_copy(target, target, sem).wait()

    def third_rows(third):
        return pl.ds(*groups[third])

    def depth_at(c):
        return pl.ds(pl.multiple_of(c * CHUNK, CHUNK), CHUNK)

    last_start = (chunks - 1) * CHUNK
    last_depth = depth - last_start
    rows_real = pl.ds(0, pair_rows)
    spare = pl.ds(pair_rows, rows.shape[1] - pair_rows)

    tails = (
        pltpu.make_async_copy(
            v_hbm.at[:, :, :, pl.ds(last_start, last_depth)], column_tail, load_sem.at[0]
        ),
        pltpu.make_async_copy(
            t_hbm.at[:, pl.ds(last_start, last_depth)], row_tail, load_sem.at[1]
        ),
        pltpu.make_async_copy(occ_hbm, occ, load_sem.at[2]),
        pltpu.make_async_copy(vir_hbm, vir, load_sem.at[3]),
    )
    barrier = pltpu.get_barrier_semaphore()
    owned[...] = jnp.zeros_like(owned)
    for step in range(1, 4):
        pl.semaphore_signal(
            barrier, inc=1, device_id={"row": (row + step) % 4}, device_id_type=MESH
        )
    for mate in (core_mate, x_mate, y_mate, cross_mate):
        pl.semaphore_signal(barrier, inc=1, device_id=mate, device_id_type=MESH)
    for copy in tails:
        copy.start()
    land[0, chunks - 1] = jnp.zeros_like(land[0, chunks - 1])
    tails[0].wait()
    land[0, chunks - 1, :, :, :, pl.ds(0, last_depth)] = column_tail[...]

    def send_far(source, c):
        @pl.when(edge)
        def _():
            remote(
                source, land.at[1, c], sent_sem.at[0], whole_sem.at[c - near],
                {"row": inner_row},
            ).start()

        @pl.when(jnp.logical_not(edge))
        def _():
            remote(
                source, land.at[2, c], sent_sem.at[0], whole_sem.at[far + c],
                {"row": far_inner},
            ).start()
            remote(
                source, land.at[1, c], sent_sem.at[1], whole_sem.at[c - near],
                {"row": edge_row},
            ).start()

    pl.semaphore_wait(barrier, 7)

    def far_loop(c, carry):
        send_far(v_hbm.at[:, :, :, depth_at(c)], c)
        return carry

    lax.fori_loop(near, chunks - 1, far_loop, 0)
    send_far(land.at[0, chunks - 1], chunks - 1)

    @pl.when(edge)
    def _():
        def send_lent(c, carry):
            remote(
                t_hbm.at[:, depth_at(c)], lent.at[c, rows_real], sent_sem.at[1],
                lent_sem.at[c], {"row": inner_row},
            ).start()
            return carry

        def send_piece(third, c, carry):
            remote(
                v_hbm.at[:, :, third_rows(third), depth_at(c)],
                land.at[1, c, :, :, third_rows(third)],
                sent_sem.at[2], third_sem.at[0, third * near + c], {"row": inner_row},
            ).start()
            return carry

        lax.fori_loop(0, near, send_lent, 0)
        for third in range(thirds):
            lax.fori_loop(0, near, functools.partial(send_piece, third), 0)

    @pl.when(jnp.logical_not(edge))
    def _():
        def send_near(c, carry):
            remote(
                v_hbm.at[:, :, :, depth_at(c)], land.at[2, c], sent_sem.at[2],
                whole_sem.at[far + c], {"row": far_inner},
            ).start()
            return carry

        lax.fori_loop(0, near, send_near, 0)

    def load_chunk(c, carry):
        pltpu.make_async_copy(
            t_hbm.at[:, depth_at(c)], rows.at[c, rows_real], load_sem.at[4]
        ).start()
        pltpu.make_async_copy(
            v_hbm.at[:, :, :, depth_at(c)], land.at[0, c], load_sem.at[5]
        ).start()
        return carry

    lax.fori_loop(0, chunks - 1, load_chunk, 0)
    acc[...] = jnp.zeros_like(acc)
    rows[chunks - 1] = jnp.zeros_like(rows[chunks - 1])

    def clear_rows(c, carry):
        rows[c, spare] = jnp.zeros_like(rows[c, spare])
        return carry

    def clear_lent(c, carry):
        lent[c, spare] = jnp.zeros_like(lent[c, spare])
        return carry

    lax.fori_loop(0, chunks - 1, clear_rows, 0)
    lax.fori_loop(0, near, clear_lent, 0)
    for copy in tails[1:]:
        copy.wait()
    rows[chunks - 1, rows_real, pl.ds(0, last_depth)] = row_tail[...]
    denominators(pair_rows, occ, vir, below)
    loaded = pl.ds(0, chunks - 1)
    arrived(rows.at[loaded, rows_real], load_sem.at[4])
    arrived(land.at[0, loaded], load_sem.at[5])

    def add_whole(block, c, pairs):
        other = split(block[c])
        for slot, part in pairs:
            columns = land[part, c].reshape(-1, CHUNK)
            acc[slot] += product(split(columns), other).reshape(acc.shape[1:])

    def add_third(block, c, third, pairs):
        other = split(block[c])
        for slot, part in pairs:
            at = third_rows(third)
            columns = land[part, c, :, :, at].reshape(-1, CHUNK)
            sums = product(split(columns), other)
            acc[slot, :, :, at] += sums.reshape(2, 2, at.size, -1)

    class Unit:
        def __init__(self, index, slots, group, here, there):
            self.index, self.slots, self.group = index, slots, group
            self.here, self.there = here, there
            self.slot_here, self.slot_there = here is not None, there is not None
            if self.slot_here and self.slot_there:
                self.kept = jnp.where(home, here, there)
                self.given = jnp.where(home, there, here)
                self.gives = self.takes = True
            else:
                self.kept = self.given = slots
                self.takes = home if self.slot_here else jnp.logical_not(home)
                self.gives = jnp.logical_not(self.takes)

        def core_copy(self):
            return remote(
                acc.at[self.slots, :, 1 - core, self.group],
                from_core.at[self.slots, :, self.group],
                hop_send.at[self.index, 0], hop_recv.at[self.index, 0], core_mate,
            )

        def x_copy(self):
            return remote(
                acc.at[self.slots, 1 - x_side, core, self.group],
                from_x.at[self.slots, self.group],
                hop_send.at[self.index, 1], hop_recv.at[self.index, 1], x_mate,
            )

        def y_copy(self):
            return remote(
                acc.at[self.given, x_side, core, self.group],
                from_y.at[self.given, self.group],
                hop_send.at[self.index, 2], hop_recv.at[self.index, 2], y_mate,
            )

        def start(self):
            self.core_copy().start()

        def second(self):
            self.core_copy().wait()
            at = (self.slots, slice(None), core, self.group)
            acc[at] += from_core[self.slots, :, self.group]
            self.x_copy().start()

        def third(self):
            self.x_copy().wait()
            acc[self.slots, x_side, core, self.group] += from_x[self.slots, self.group]
            when(self.gives, lambda: self.y_copy().start())

        def last(self, targets_here, targets_there=()):
            when(self.gives, lambda: self.y_copy().wait_send())

            def take():
                self.y_copy().wait_recv()
                at = (self.kept, x_side, core, self.group)
                acc[at] += from_y[self.kept, self.group]

            when(self.takes, take)

            self.deliver(targets_here, targets_there)

        def deliver(self, targets_here, targets_there=()):
            def go(targets):
                for slot, target, device, send, recv in targets:
                    source = acc.at[slot, x_side, core, self.group]
                    if device is None:
                        target[self.group] = source[...]
                    else:
                        remote(
                            source, target.at[self.group], home_send.at[send], recv,
                            {"row": device},
                        ).start()

            if targets_here:
                pl.when(home)(lambda: go(targets_here))
            if targets_there:
                pl.when(jnp.logical_not(home))(lambda: go(targets_there))

        def cross_copy(self):
            return remote(
                acc.at[self.slots, 1 - x_side, core, self.group], from_cross,
                cross_sem.at[0], cross_sem.at[1], cross_mate,
            )

        def scatter(self):
            self.core_copy().wait()
            at = (self.slots, slice(None), core, self.group)
            acc[at] += from_core[self.slots, :, self.group]
            when(home, lambda: self.x_copy().start())

            @pl.when(jnp.logical_not(home))
            def _():
                self.cross_copy().start()
                self.y_copy().start()

        def gather(self, targets):
            @pl.when(home)
            def _():
                self.x_copy().wait()
                self.y_copy().wait_recv()
                at = (self.slots, x_side, core, self.group)
                near_sum = from_x[self.slots, self.group] + from_y[self.slots, self.group]
                self.cross_copy().wait_recv()
                acc[at] += near_sum + from_cross[...]

            @pl.when(jnp.logical_not(home))
            def _():
                self.y_copy().wait_send()
                self.cross_copy().wait_send()

            self.deliver(targets)

        def run(self, targets_here, targets_there=()):
            self.start()
            self.second()
            self.third()
            self.last(targets_here, targets_there)

    def when(condition, action):
        if condition is True:
            action()
        else:
            pl.when(condition)(action)

    every = pl.ds(0, slab)

    def owned_whole(kind):
        arrived(owned.at[kind, every], kind_sem(kind, 0))

    def owned_third(kind, third):
        arrived(owned.at[kind, third_rows(third)], kind_sem(kind, third))

    def put(block, at, value):
        lanes = pl.ds(block * pair_rows, pair_rows)
        real = slice(0, pair_rows)
        out[0, at, lanes] = value[:, real]
        out[1, at, lanes] = (value / below[block, at])[:, real]

    def put_edge(at):
        for block in range(2):
            pl.when(col == block)(lambda: put(block, at, owned[0, at] + owned[2, at]))

    def put_inner(at):
        for block in range(2):
            pl.when(col != block)(lambda: put(block, at, owned[1, at]))

    def kind_sem(kind, group):
        return home_recv.at[kind * thirds + group]

    @pl.when(edge)
    def _():
        def own(c, carry):
            add_whole(rows, c, ((0, 0),))
            return carry

        def other(part, i, carry):
            c = near + i
            first = (0, far + near, far + chunks)[part - 1]
            arrived(land.at[part, c], whole_sem.at[first + i])
            add_whole(rows, c, ((part, part),))
            return carry

        lax.fori_loop(0, chunks, own, 0)
        lax.fori_loop(0, far, functools.partial(other, 1), 0)
        Unit(0, pl.ds(0, 2), every, 0, None).run(
            (
                (0, owned.at[0], None, 0, None),
                (1, owned.at[0], inner_row, 0, kind_sem(0, 0)),
            )
        )
        lax.fori_loop(0, far, functools.partial(other, 2), 0)
        second_unit = Unit(1, pl.ds(2, 1), every, None, 2)
        second_unit.run(())
        lax.fori_loop(0, far, functools.partial(other, 3), 0)
        Unit(2, pl.ds(3, 1), every, 3, None).run(())
        pl.semaphore_wait(go_sem, 1)
        second_unit.deliver(
            ((3, owned.at[0], far_edge, 2, kind_sem(0, 0)),),
            ((2, relay.at[0], far_inner, 1, relay_recv.at[0]),),
        )

        def sent_home(send, group):
            remote(
                acc.at[0, x_side, core, group], owned.at[0, group],
                home_send.at[send], home_recv.at[0], {"row": inner_row},
            ).wait_send()

        @pl.when(home)
        def _():
            sent_home(0, every)
            sent_home(2, every)

        @pl.when(jnp.logical_not(home))
        def _():
            sent_home(1, every)

        arrived_far = pl.ds(near, far)
        for at, source in (
            (0, land.at[0, arrived_far]), (2, land.at[0, pl.ds(0, near)]),
        ):
            remote(
                source, source, sent_sem.at[at], whole_sem.at[0], {"row": inner_row}
            ).wait_send()
        remote(
            rows.at[pl.ds(0, near), rows_real], rows.at[pl.ds(0, near), rows_real],
            sent_sem.at[1], whole_sem.at[0], {"row": inner_row},
        ).wait_send()

    @pl.when(jnp.logical_not(edge))
    def _():
        def first_far(i, carry):
            c = near + i
            arrived(land.at[1, c], whole_sem.at[c - near])
            remote(
                land.at[1, c], land.at[3, c], sent_sem.at[3], whole_sem.at[far + chunks + c - near],
                {"row": far_inner},
            ).start()
            arrived(land.at[2, c], whole_sem.at[far + c])
            remote(
                land.at[2, c], land.at[2, c], sent_sem.at[4], whole_sem.at[far + c],
                {"row": edge_row},
            ).start()
            add_whole(rows, c, ((0, 0), (4, 1), (1, 2)))
            return carry

        def first_near(c, carry):
            arrived(land.at[2, c], whole_sem.at[far + c])
            add_whole(rows, c, ((0, 0), (1, 2)))
            return carry

        def lent_chunk(c, carry):
            arrived(lent.at[c, rows_real], lent_sem.at[c])
            add_whole(lent, c, ((2, 0), (3, 2)))
            return carry

        def second_far(c, carry):
            arrived(land.at[3, c], whole_sem.at[far + chunks + c - near])
            remote(
                land.at[3, c], land.at[3, c], sent_sem.at[5], whole_sem.at[far + chunks + c - near],
                {"row": edge_row},
            ).start()
            add_whole(rows, c, ((5, 3),))
            return carry

        lax.fori_loop(0, far, first_far, 0)

        def lent_due(step):
            due = (8 * step - 1) // 21
            return jnp.where(step < 1, 0, jnp.minimum(due, near))

        def with_lent(body, step, carry):
            body(step, carry)
            count = lent_due(step)

            @pl.when(count > lent_due(step - 1))
            def _():
                lent_chunk(count - 1, 0)

            return carry

        lax.fori_loop(0, near, functools.partial(with_lent, first_near), 0)
        own_unit = Unit(0, pl.ds(0, 2), every, 0, 1)
        own_unit.run(((0, owned.at[1], None, 0, None),))
        lax.fori_loop(near, chunks, functools.partial(with_lent, second_far), 0)
        left = near - (8 * (chunks - 1) - 1) // 21
        for j in range(max(left, 0)):
            lent_chunk(near - left + j, 0)

        lent_unit = Unit(1, pl.ds(2, 2), every, 2, 3)
        own_targets = ((1, relay.at[1], far_inner, 0, relay_recv.at[1]),)
        lent_targets = ((3, relay.at[2], far_inner, 1, relay_recv.at[2]),)

        def edge_unit(third):
            return Unit(2 + third, pl.ds(4, 1), third_rows(third), 4, None)

        def edge_targets(third):
            return ((4, owned.at[1], edge_row, 2 + third, kind_sem(1, third)),)

        def last_unit(third):
            return Unit(2 + thirds + third, pl.ds(5, 2), third_rows(third), 5, None)

        def last_targets(third):
            return (
                (5, owned.at[1], far_edge, 2 + thirds + third, kind_sem(1, third)),
                (6, owned.at[2], far_edge, 2 + 2 * thirds + third, kind_sem(2, third)),
            )

        def pass_on(third, c):
            n = third * near + c
            at = third_rows(third)
            arrived(land.at[1, c, :, :, at], third_sem.at[0, n])
            remote(
                land.at[1, c, :, :, at], land.at[3, c, :, :, at],
                sent_sem.at[6], third_sem.at[1, n], {"row": far_inner},
            ).start()
            add_third(rows, c, third, ((4, 1),))

        def near_step(third, c, carry):
            ahead = c + LAG
            pl.when(ahead < near)(lambda: pass_on(third, ahead))
            if third + 1 < thirds:
                pl.when(ahead >= near)(lambda: pass_on(third + 1, ahead - near))
            at = third_rows(third)
            arrived(land.at[3, c, :, :, at], third_sem.at[1, third * near + c])
            add_third(rows, c, third, ((5, 3),))
            add_third(lent, c, third, ((6, 3),))

            def stage(step, action):
                pl.when(c == step)(action)

            if third == 0:
                stage(0, lent_unit.start)
                stage(2, lent_unit.second)
                stage(6, lent_unit.third)
                stage(10, lambda: lent_unit.last(((2, owned.at[2], None, 0, None),)))
            else:
                before = third - 1
                late = before + 2 == thirds
                stage(0, last_unit(before).start)
                stage(2, last_unit(before).second)
                stage(7, last_unit(before).third)
                if not late:
                    stage(near - 1, lambda: last_unit(before).last(()))
                stage(1, edge_unit(before).third)
                stage(5, lambda: edge_unit(before).last(edge_targets(before)))
            stage(near - LAG, edge_unit(third).start)
            stage(near - LAG + 2, edge_unit(third).second)
            if third + 1 == thirds:
                stage(near - LAG, cross)
            return carry

        def cross():
            pl.semaphore_signal(
                go_sem, inc=1, device_id={"row": edge_row}, device_id_type=MESH
            )
            own_unit.deliver((), own_targets)
            lent_unit.deliver((), lent_targets)
            for third in range(thirds - 2):
                last_unit(third).deliver(last_targets(third))

        def send_relay(kind):
            return remote(
                relay.at[kind], owned.at[kind], home_send.at[2 + 3 * thirds + kind],
                kind_sem(kind, 0), y_mate,
            )

        def relay_on(kind):
            @pl.when(home)
            def _():
                arrived(relay.at[kind], relay_recv.at[kind])
                send_relay(kind).start()

        for c in range(LAG):
            pass_on(0, c)
        for third in range(thirds):
            lax.fori_loop(0, near, functools.partial(near_step, third), 0)
        final = thirds - 1
        last_unit(final).start()
        edge_unit(final).third()
        last_unit(final - 1).last(last_targets(final - 1))
        last_unit(final).scatter()

        @pl.when(home)
        def _():
            owned_whole(0)
            put_edge(every)
            put_inner(every)

        relay_on(1)
        edge_unit(final).last(edge_targets(final))

        @pl.when(home)
        def _():
            for kind in (2, 0):
                arrived(relay.at[kind], relay_recv.at[kind])
            relay[2] += relay[0]
            send_relay(2).start()

        last_unit(final).gather(last_targets(final))

        def sent_home(send, group):
            remote(
                acc.at[0, x_side, core, group], owned.at[1, group],
                home_send.at[send], home_recv.at[0], {"row": far_inner},
            ).wait_send()

        @pl.when(home)
        def _():
            for at in range(3):
                for third in range(thirds):
                    sent_home(2 + at * thirds + third, third_rows(third))
            for kind in (1, 2):
                send_relay(kind).wait_send()

        @pl.when(jnp.logical_not(home))
        def _():
            sent_home(0, every)
            sent_home(1, every)

        arrived_far = pl.ds(near, far)
        arrived_near = pl.ds(0, near)
        for at, source in (
            (0, land.at[0, arrived_far]),
            (1, land.at[0, arrived_far]),
            (2, land.at[0, arrived_near]),
            (3, land.at[1, arrived_far]),
            (4, land.at[2, arrived_far]),
            (5, land.at[3, arrived_far]),
            (6, land.at[1, arrived_near]),
        ):
            remote(
                source, source, sent_sem.at[at], whole_sem.at[0], {"row": far_inner}
            ).wait_send()

    @pl.when(edge & home)
    def _():
        put_edge(every)
        for third in range(thirds):
            owned_third(1, third)
            put_inner(third_rows(third))

    @pl.when(edge & jnp.logical_not(home))
    def _():
        owned_whole(0)
        for third in range(thirds):
            owned_third(1, third)
            put_inner(third_rows(third))
            owned_third(2, third)
            put_edge(third_rows(third))

    @pl.when(jnp.logical_not(edge) & jnp.logical_not(home))
    def _():
        owned_whole(1)
        put_inner(every)
        owned_whole(2)
        put_edge(every)


def line_exchange(amplitudes, integrals, occ_energy, vir_energy):
    pair_rows = amplitudes.shape[0]
    depth, width = integrals.shape
    chunks = -(-depth // CHUNK)
    near = near_chunks(chunks)
    layers = lax.axis_size("layer")
    slab = width // layers
    groups = groups_of(slab)
    thirds = len(groups)
    padded = -(-pair_rows // 128) * 128
    last_depth = depth - (chunks - 1) * CHUNK
    vmem = functools.partial(pltpu.VMEM, dtype=jnp.float32)
    smem = functools.partial(pltpu.SMEM, dtype=jnp.float32)
    dma = pltpu.SemaphoreType.DMA
    flops = 2 * 3 * 5 * pair_rows * depth * width
    columns = integrals.T.reshape(layers // 2, 2, slab, depth)
    result = pl.pallas_call(
        functools.partial(line_kernel, near),
        out_shape=jax.ShapeDtypeStruct((2, slab, 2 * pair_rows), jnp.float32),
        in_specs=[pl.BlockSpec(memory_space=pl.ANY)] * 4,
        out_specs=pl.BlockSpec(memory_space=pltpu.VMEM),
        scratch_shapes=[
            vmem((chunks, padded, CHUNK)),
            vmem((near, padded, CHUNK)),
            vmem((4, chunks, 2, 2, slab, CHUNK)),
            vmem((7, 2, 2, slab, padded)),
            vmem((7, 2, slab, padded)),
            vmem((7, slab, padded)),
            vmem((7, slab, padded)),
            vmem((2, groups[-1][1], padded)),
            vmem((3, slab, padded)),
            vmem((3, slab, padded)),
            vmem((2, slab, padded)),
            vmem((pair_rows, last_depth)),
            vmem((2, 2, slab, last_depth)),
            smem(occ_energy.shape),
            smem(vir_energy.shape),
            dma((6,)),
            dma((3 * chunks - 2 * near,)),
            dma((2, near * thirds)),
            dma((near,)),
            dma((7,)),
            dma((2 + 2 * thirds, 3)),
            dma((2 + 2 * thirds, 3)),
            dma((2,)),
            dma((5 + 3 * thirds,)),
            dma((3 * thirds,)),
            dma((3,)),
            pltpu.SemaphoreType.REGULAR,
        ],
        compiler_params=pltpu.CompilerParams(
            collective_id=0, has_side_effects=True, vmem_limit_bytes=67043328
        ),
        cost_estimate=pl.CostEstimate(
            flops=flops, bytes_accessed=4 * depth * (pair_rows + width), transcendentals=0
        ),
    )(amplitudes, columns, occ_energy, vir_energy)
    return result[0].T, result[1].T


def gathered(amplitudes, integrals):
    partial_rows = jnp.dot(
        amplitudes,
        lax.all_gather(integrals, "row", axis=1, tiled=True),
        precision=lax.Precision.HIGHEST,
        preferred_element_type=jnp.float32,
    )
    partial_sum = lax.all_to_all(partial_rows, "row", split_axis=1, concat_axis=0, tiled=True)
    return lax.psum_scatter(
        owner_blocks(partial_sum), ("col", "layer"), scatter_dimension=0, tiled=True
    )


def fits_line(amplitudes, integrals):
    pair_rows = amplitudes.shape[0]
    depth, width = integrals.shape
    chunks = -(-depth // CHUNK)
    near = near_chunks(chunks)
    even = width % 32 == 0 and width >= 128 and pair_rows % 8 == 0
    words = chunks * (4 * width + pair_rows) + near * pair_rows
    return even and near >= 13 and words * CHUNK * 4 < 56 * 2**20


def shards(amplitudes, integrals, occ_energy, vir_energy):
    in_line = lax.axis_size("row") == 4 and lax.axis_size("col") == 2
    in_line = in_line and lax.axis_size("layer") == 4
    if in_line and fits_line(amplitudes, integrals):
        return line_exchange(amplitudes, integrals, occ_energy, vir_energy)
    ladder = gathered(amplitudes, integrals)
    pair_rows = ladder.shape[0]
    slab_cols = ladder.shape[1]
    occupied = occ_energy.shape[0]
    virtuals = vir_energy.shape[0]
    first_np, second_np = np.triu_indices(occupied, 1)
    ij_start = lax.axis_index("col") * pair_rows
    ab_start = (
        lax.axis_index("row") * lax.axis_size("layer") + lax.axis_index("layer")
    ) * slab_cols
    first_index = lax.dynamic_slice_in_dim(
        jnp.asarray(first_np, dtype=jnp.int32), ij_start, pair_rows
    )
    second_index = lax.dynamic_slice_in_dim(
        jnp.asarray(second_np, dtype=jnp.int32), ij_start, pair_rows
    )
    pair_sum = lookup(first_index, occ_energy) + lookup(second_index, occ_energy)
    ab_index = ab_start + jnp.arange(slab_cols, dtype=jnp.int32)
    vir_sum = lookup(ab_index // virtuals, vir_energy) + lookup(ab_index % virtuals, vir_energy)
    denominator = pair_sum[:, None] - vir_sum[None, :]
    return (ladder, ladder / denominator)


def solution(mesh):
    in_specs = (P("row", ("layer", "col")), P(("layer", "col"), "row"), P(), P())
    out_specs = (P("col", ("row", "layer")), P("col", ("row", "layer")))
    return jax.shard_map(shards, mesh=mesh, in_specs=in_specs, out_specs=out_specs, check_vma=False)
```
